128 devices in a mesh: rx: 16 (over x_lo, z, core), ry: 8 (over x_hi, y).
Axes of the slice: x: 4 (x_hi: 2, x_lo: 2; x = x_hi * 2 + x_lo), y: 4, z: 4, core: 2. Of those that a mesh axis runs over, the one named last changes fastest.
Arguments:
- record: bfloat16 [512, 512, 2048], P('rx', 'ry'), may hold values from -6 to 6
- sampled: int32 [512, 512], P('rx', 'ry'), may hold values 0 or 1
- levels: int32 [2], replicated, may hold values from 40 to 160
Outputs:
- restored: bfloat16 [512, 512, 2048], P('rx', 'ry')
The draws below stay inside these ranges and needn't reach their ends.
All inputs are finite; a program needn't handle non-finite values. No bound on the sum of `sampled` on one device may be relied on, other than what follows from the above.
Results may differ from the reference program's by a relative error of at most 0.0027.
Values may be sent and summed in bfloat16 or wider, within the bound.
No kernel may reach another device: no remote copies, remote signals or barrier semaphores. Data moves between devices by JAX's collectives and lax.ppermute only.
A program may use at most 128 MiB of HBM per device.

```python
import math
import jax
import jax.numpy as jnp
from jax import lax

CX = 32
CY = 64
H = 16
NT = 2048
NF = 128
FLO = 8
ITERS = 2
RX = 512
RY = 512
N_RX = 16


def set_ends(values, key, least, top_value):
    index_at = [jax.random.randint(jax.random.fold_in(key, axis), (), 0, length) for axis, length in enumerate(values.shape)]
    widest = values.shape.index(max(values.shape))
    next_to = index_at[:widest] + [(index_at[widest] + 1) % values.shape[widest]] + index_at[widest + 1:]
    return values.at[tuple(index_at)].set(least).at[tuple(next_to)].set(top_value)


def steps_of(key, shape, split, low, top_value):
    def one(axis_at, shards_of):
        steps = jax.random.uniform(jax.random.fold_in(jax.random.fold_in(key, 6), axis_at), (shards_of,), jnp.float32, low / len(split), top_value / len(split))
        return jnp.repeat(jnp.exp(steps), shape[axis_at] // shards_of).reshape((-1,) + (1,) * (len(shape) - axis_at - 1))

    gain = one(*split[0])
    for cut in split[1:]:
        gain = gain * one(*cut)
    return gain


def noise(stream_key, shape, width, bound, cuts=(), dtype=jnp.bfloat16):
    entries = width * jax.random.normal(stream_key, shape, jnp.float32)
    if cuts:
        entries = entries * steps_of(stream_key, shape, cuts, -0.22, 0.18)
    return jnp.clip(entries, -bound, bound).astype(dtype)


def setup_inputs(seed: int = 0) -> dict:
    arg_keys = jax.random.split(jax.random.key(seed), 4)
    return {
        "record": noise(arg_keys[0], (RX, RY, NT), 1.0, 6.0, ((0, 16), (1, 8))),
        "sampled": set_ends((jax.random.randint(arg_keys[1], (RX, RY), 0, 2) < 1).astype(jnp.int32), jax.random.fold_in(arg_keys[1], 1), 0, 1),
        "levels": jax.random.randint(arg_keys[2], (ITERS,), 40, 161).astype(jnp.int32),
    }


def angles(row_ids, column_ids, period):
    products = row_ids[:, None] * column_ids[None, :] % period
    return products.astype(jnp.float32) * (2.0 * math.pi / period)

def taper(interior, margin):
    offsets = jnp.arange(interior + 2 * margin).astype(jnp.float32)
    rising = jnp.sin(0.5 * math.pi * (offsets + 0.5) / (2 * margin))
    falling = jnp.cos(0.5 * math.pi * (offsets - interior + 0.5) / (2 * margin))
    return jnp.where(offsets < 2 * margin, rising, jnp.where(offsets >= interior, falling, jnp.ones_like(offsets)))

def time_forward(samples, bin_ids):
    phases = angles(jnp.arange(samples), bin_ids, samples)
    return jnp.stack([jnp.cos(phases), -jnp.sin(phases)], axis=1).astype(jnp.bfloat16)

def time_inverse(samples, bin_ids):
    phases = angles(bin_ids, jnp.arange(samples), samples)
    factor = 2.0 / samples
    return jnp.stack([jnp.cos(phases) * factor, -jnp.sin(phases) * factor], axis=1).astype(jnp.bfloat16)

def tile_forward(interior, margin):
    length = interior + 2 * margin
    offsets = jnp.arange(length)
    phases = angles(offsets, offsets, length)
    weights = taper(interior, margin)[None, :]
    cosine = (weights * jnp.cos(phases)).astype(jnp.bfloat16)
    sine_table = (weights * jnp.sin(phases)).astype(jnp.bfloat16)
    real_rows = jnp.stack([cosine, sine_table], axis=1)
    imag_rows = jnp.stack([-sine_table, cosine], axis=1)
    return jnp.stack([real_rows, imag_rows], axis=0)

def tile_inverse(interior, margin):
    length = interior + 2 * margin
    offsets = jnp.arange(length)
    phases = angles(offsets, offsets, length)
    weights = (taper(interior, margin) * (1.0 / length))[:, None]
    cosine = (weights * jnp.cos(phases)).astype(jnp.bfloat16)
    sine_table = (weights * jnp.sin(phases)).astype(jnp.bfloat16)
    real_rows = jnp.stack([cosine, -sine_table], axis=1)
    imag_rows = jnp.stack([sine_table, cosine], axis=1)
    return jnp.stack([real_rows, imag_rows], axis=0)

def plane_forward(positions, halves, length):
    columns = jnp.arange(2 * length)
    phases = angles(positions, columns % length, length)
    matched = halves[:, None] == (columns // length)[None, :]
    signed = jnp.where(halves[:, None] == 0, -1.0, 1.0) * jnp.sin(phases)
    return jnp.where(matched, jnp.cos(phases), signed).astype(jnp.bfloat16)

def plane_inverse(positions, halves, length):
    rows_all = jnp.arange(2 * length)
    phases = angles(rows_all % length, positions, length)
    factor = 1.0 / length
    matched = (rows_all // length)[:, None] == halves[None, :]
    signed = jnp.where((rows_all // length)[:, None] == 0, 1.0, -1.0) * (jnp.sin(phases) * factor)
    return jnp.where(matched, jnp.cos(phases) * factor, signed).astype(jnp.bfloat16)

def intersection_add(pieces, interior, margin):
    middle = pieces[:, :, margin:margin + interior].astype(jnp.float32)
    from_left = jnp.roll(pieces[:, :, interior + margin:], 1, axis=1).astype(jnp.float32)
    from_right = jnp.roll(pieces[:, :, :margin], -1, axis=1).astype(jnp.float32)
    filler = jnp.zeros(middle.shape[:2] + (interior - 2 * margin,) + middle.shape[3:], jnp.float32)
    extra = jnp.concatenate([from_left, filler, from_right], axis=2)
    return (middle + extra).astype(jnp.bfloat16)

def reference(record, sampled, levels):
    bin_ids = FLO + jnp.arange(NF)
    forward_time = time_forward(NT, bin_ids).astype(jnp.float32)
    inverse_time = time_inverse(NT, bin_ids).astype(jnp.float32)
    forward_tile = tile_forward(CY, H).astype(jnp.float32)
    inverse_tile = tile_inverse(CY, H).astype(jnp.float32)
    positions = jnp.concatenate([jnp.arange(RX), jnp.arange(RX)])
    halves = jnp.concatenate([jnp.zeros(RX, jnp.int32), jnp.ones(RX, jnp.int32)])
    forward_plane = plane_forward(positions, halves, RX).astype(jnp.float32)
    inverse_plane = plane_inverse(positions, halves, RX).astype(jnp.float32)
    tiles_count = RY // CY
    length = CY + 2 * H
    current = jnp.where(sampled[:, :, None] > 0, record, jnp.zeros((), jnp.bfloat16))
    record_blocks = record.reshape(N_RX, CX, RY, NT)
    kept_blocks = sampled.astype(jnp.float32).reshape(N_RX, CX, RY, 1)

    def spectrum(row_block):
        return jnp.einsum('xyt,tpf->fypx', row_block.astype(jnp.float32), forward_time).astype(jnp.bfloat16)

    def rebuild(operands):
        column_piece, initial, kept = operands
        recon = jnp.einsum('fypx,fpt->xyt', column_piece.astype(jnp.float32), inverse_time)
        return (kept * initial.astype(jnp.float32) + (1.0 - kept) * recon).astype(jnp.bfloat16)
    for iteration in range(ITERS):
        spectra = lax.map(spectrum, current.reshape(N_RX, CX, RY, NT))
        spectra = jnp.transpose(spectra, (1, 2, 3, 0, 4)).reshape(NF, tiles_count, CY, 2, RX)
        leading = jnp.roll(spectra, 1, axis=1)[:, :, CY - H:]
        trailing = jnp.roll(spectra, -1, axis=1)[:, :, :H]
        windows = jnp.concatenate([leading, spectra, trailing], axis=2)
        turned = jnp.einsum('qkps,fjspx->fjkqx', forward_tile, windows.astype(jnp.float32)).astype(jnp.bfloat16)
        coeffs = jnp.dot(turned.reshape(-1, 2 * RX).astype(jnp.float32), forward_plane, preferred_element_type=jnp.float32)
        real_part = coeffs[:, :RX]
        imag_part = coeffs[:, RX:]
        magnitude = jnp.sqrt(real_part * real_part + imag_part * imag_part)
        largest = jnp.max(magnitude)
        cutoff = levels[iteration].astype(jnp.float32) * 0.001 * (largest + 1e-06)
        shrink = jnp.maximum(magnitude - cutoff, 0.0) / jnp.maximum(magnitude, cutoff)
        shrunk = (coeffs * jnp.concatenate([shrink, shrink], axis=1)).astype(jnp.bfloat16)
        planes = jnp.dot(shrunk.astype(jnp.float32), inverse_plane, preferred_element_type=jnp.float32)
        planes = planes.astype(jnp.bfloat16).reshape(NF, tiles_count, length, 2, RX)
        pieces = jnp.einsum('qspk,fjkpx->fjsqx', inverse_tile, planes.astype(jnp.float32)).astype(jnp.bfloat16)
        merged = intersection_add(pieces, CY, H).reshape(NF, RY, 2, N_RX, CX)
        column_pieces = jnp.moveaxis(merged, 3, 0)
        current = lax.map(rebuild, (column_pieces, record_blocks, kept_blocks)).reshape(RX, RY, NT)
    return current
```

```python
import functools

import jax
import jax.numpy as jnp
import numpy as np
from jax import lax
from jax.experimental import pallas as pl
from jax.experimental.pallas import tpu as pltpu
from jax.sharding import Mesh
from jax.sharding import PartitionSpec as P

H = 16
NF = 128
FLO = 8
CX, CY, NT = 32, 64, 2048
LX = 512
HALF = LX // 2
TILES = 8
WIN = CY + 2 * H
NRX = LX // CX
ALL = ("rx_0", "rx_1", "rx_2", "ry_0", "ry_1")
F32 = jnp.float32
BF16 = jnp.bfloat16
PAD = 264
PAD3 = 40


def time_table():
    f = FLO + np.arange(NF)[:, None]
    ang = 2.0 * np.pi * (f * np.arange(NT)[None, :] % NT) / NT
    return np.concatenate([np.cos(ang), -np.sin(ang)], axis=0)


def plane_tables():
    n = np.arange(HALF)
    ang = 2.0 * np.pi * (n[:, None] * n[None, :] % HALF) / HALF
    c, s = np.cos(ang), np.sin(ang)
    forward = np.block([[c, s], [-s, c]])
    inverse = np.block([[c, -s], [s, c]]) / LX
    return forward, inverse


def twiddle_table():
    ang = 2.0 * np.pi * np.arange(HALF)[:, None] / LX
    ones = np.ones((HALF, CY))
    real = np.concatenate([ones, np.cos(ang) * ones], axis=1)
    imag = np.concatenate([0.0 * ones, -np.sin(ang) * ones], axis=1)
    return np.concatenate([real, imag], axis=0)


def taper():
    s = np.arange(WIN)
    rising = np.sin(0.5 * np.pi * (s + 0.5) / (2 * H))
    falling = np.cos(0.5 * np.pi * (s - CY + 0.5) / (2 * H))
    return np.where(s < 2 * H, rising, np.where(s >= CY, falling, 1.0))


def column_of(part, half, k):
    place = half * WIN + k
    if place < 128:
        return part * 256 + place
    return 128 + part * 64 + place - 128


def window_tables():
    k = np.arange(WIN)
    ang = 2.0 * np.pi * (k[:, None] * k[None, :] % WIN) / WIN
    w = taper()
    ya, yb = w[None, :] * np.cos(ang), w[None, :] * np.sin(ang)
    yc, yd = w[:, None] / WIN * np.cos(ang), w[:, None] / WIN * np.sin(ang)
    fwd = np.zeros((512, 384))
    inv = np.zeros((384, 512))
    for half in range(2):
        cols = [[column_of(p, half, kk) for kk in range(WIN)] for p in range(2)]
        for y in range(CY):
            spots = [(0, y + H)]
            if y < H:
                spots.append((256, CY + H + y))
            if y >= CY - H:
                spots.append((256, y - (CY - H)))
            for base, s in spots:
                re = base + half * CY + y
                im = re + 128
                fwd[re, cols[0]] = ya[:, s]
                fwd[im, cols[0]] = yb[:, s]
                fwd[im, cols[1]] = ya[:, s]
                fwd[re, cols[1]] = -yb[:, s]
                inv[cols[0], re] = yc[s, :]
                inv[cols[1], re] = -yd[s, :]
                inv[cols[1], im] = yc[s, :]
                inv[cols[0], im] = yd[s, :]
    return fwd, inv


def spectra_kernel(record_ref, mask_ref, table_ref, out_ref, hold_ref):
    step = pl.program_id(0)
    traces = record_ref[...].reshape(-1, NT)
    res = lax.dot_general(
        table_ref[...], traces, (((1,), (1,)), ((), ())), preferred_element_type=F32
    )
    blocks = res.shape[1] // 128
    for b in range(blocks):
        row = step * blocks + b
        kept = mask_ref[pl.ds(row, 1), :]
        value = jnp.where(kept > 0, res[:, b * 128 : (b + 1) * 128], 0.0)
        hold_ref[pl.ds(pl.multiple_of(row * PAD, 8), 2 * NF), :] = value

    @pl.when(step == pl.num_programs(0) - 1)
    def _():
        flag = mask_ref[...].astype(BF16)
        for f in range(NF):
            for p in range(2):
                part = hold_ref[pl.ds(p * NF + f, 16, stride=PAD), :]
                out_ref[f, p * 16 : (p + 1) * 16, :] = part.astype(BF16)
            out_ref[f, 32:48, :] = flag


def spectra_of(record, flags, table):
    rows = 4
    return pl.pallas_call(
        spectra_kernel,
        grid=(CX // rows,),
        in_specs=[
            pl.BlockSpec((rows, CY, NT), lambda i: (i, 0, 0)),
            pl.BlockSpec((16, 128), lambda i: (0, 0)),
            pl.BlockSpec((2 * NF, NT), lambda i: (0, 0)),
        ],
        out_specs=pl.BlockSpec((NF, 48, 128), lambda i: (0, 0, 0)),
        out_shape=jax.ShapeDtypeStruct((NF, 48, 128), BF16),
        scratch_shapes=[pltpu.VMEM((16 * PAD, 128), F32)],
        name="spectra",
    )(record, flags, table)


def lane_signs(shape):
    lane = lax.broadcasted_iota(jnp.int32, shape, 1)
    return jnp.where(lane % 128 < CY, 1.0, -1.0).astype(F32)


def forward_columns(data, fx_ref, tw_ref, v_ref, ry):
    res = jnp.dot(fx_ref[...], data, preferred_element_type=F32)
    xr, xi = res[:HALF], res[HALF:]
    tr, ti = tw_ref[:HALF], tw_ref[HALF:]
    sign = lane_signs((HALF, 128))
    for b in range(2):
        ar, ai = xr[:, b * 128 : (b + 1) * 128], xi[:, b * 128 : (b + 1) * 128]
        br = ar * tr - ai * ti
        bi = ar * ti + ai * tr
        at = (ry + b) * 128
        v_ref[0, :, at : at + 128] = (pltpu.roll(br, CY, 1) + br * sign).astype(BF16)
        v_ref[1, :, at : at + 128] = (pltpu.roll(bi, CY, 1) + bi * sign).astype(BF16)


def forward_tiles(v_ref, wf_ref, c_ref):
    early = lax.broadcasted_iota(jnp.int32, (HALF, 128), 1) % CY < CY // 2
    best = jnp.zeros((HALF, 128), F32)
    for j in range(TILES):
        left, right = (j - 1) % TILES * 128, (j + 1) % TILES * 128
        own = [v_ref[p, :, j * 128 : (j + 1) * 128] for p in range(2)]
        near = [
            jnp.where(early, v_ref[p, :, right : right + 128], v_ref[p, :, left : left + 128])
            for p in range(2)
        ]
        c = jnp.dot(
            jnp.concatenate(own + near, axis=1), wf_ref[...], preferred_element_type=F32
        )
        c_ref[j] = c
        c0, c1, c2 = c[:, :128], c[:, 128:256], c[:, 256:]
        sq = c1 * c1
        best = jnp.maximum(best, jnp.maximum(c0 * c0 + c2 * c2, sq + pltpu.roll(sq, CY, 1)))
    return best


def put_largest(best, top_ref):
    top = jnp.sqrt(jnp.max(best, keepdims=True))
    top_ref[...] = jnp.broadcast_to(top.reshape(1, 1, 1), top_ref.shape)


def shrink_tiles(c_ref, tops_ref, level, wi_ref, o_ref):
    tau = level.astype(F32) * 0.001 * (jnp.max(tops_ref[...]) + 1e-06)
    for j in range(TILES):
        c = c_ref[j]
        c0, c1, c2 = c[:, :128], c[:, 128:256], c[:, 256:]
        sq = c1 * c1
        g0 = jnp.maximum(1.0 - tau * lax.rsqrt(c0 * c0 + c2 * c2), 0.0)
        g1 = jnp.maximum(1.0 - tau * lax.rsqrt(sq + pltpu.roll(sq, CY, 1)), 0.0)
        e = jnp.concatenate([c0 * g0, c1 * g1, c2 * g0], axis=1).astype(BF16)
        o_ref[j] = jnp.dot(e, wi_ref[...], preferred_element_type=F32)


def inverse_columns(o_ref, ix_ref, tw_ref, ry):
    tr, ti = tw_ref[:HALF], tw_ref[HALF:]
    sign = lane_signs((HALF, 128))
    early = lax.broadcasted_iota(jnp.int32, (HALF, 128), 1) % CY < CY // 2
    reals, imags = [], []
    for j in (ry, ry + 1):
        left, right = (j - 1) % TILES, (j + 1) % TILES
        parts = []
        for p in range(2):
            own = o_ref[j, :, p * 128 : (p + 1) * 128]
            at = 256 + p * 128
            near = jnp.where(early, o_ref[left, :, at : at + 128], o_ref[right, :, at : at + 128])
            both = own + near
            parts.append(pltpu.roll(both, CY, 1) + both * sign)
        reals.append(parts[0] * tr + parts[1] * ti)
        imags.append(parts[1] * tr - parts[0] * ti)
    g = jnp.concatenate(
        [jnp.concatenate(reals, axis=1), jnp.concatenate(imags, axis=1)], axis=0
    ).astype(BF16)
    return jnp.dot(ix_ref[...], g, preferred_element_type=F32)


def columns_of(in_ref, ry):
    return [
        in_ref[:, ry, p * 16 : (p + 1) * 16, :].reshape(HALF, 128) for p in range(2)
    ]


def first_kernel(in_ref, fx_ref, tw_ref, wf_ref, c_ref, top_ref, v_ref):
    for ry in range(0, TILES, 2):
        a, b = columns_of(in_ref, ry), columns_of(in_ref, ry + 1)
        data = jnp.concatenate(
            [jnp.concatenate([a[p], b[p]], axis=1) for p in range(2)], axis=0
        )
        forward_columns(data, fx_ref, tw_ref, v_ref, ry)
    put_largest(forward_tiles(v_ref, wf_ref, c_ref), top_ref)


def middle_kernel(
    level_ref, c_ref, tops_ref, in_ref, fx_ref, ix_ref, tw_ref, wf_ref, wi_ref,
    c2_ref, top_ref, o_ref, v_ref,
):
    shrink_tiles(c_ref, tops_ref, level_ref[0], wi_ref, o_ref)
    for ry in range(0, TILES, 2):
        z = inverse_columns(o_ref, ix_ref, tw_ref, ry)
        a, b = columns_of(in_ref, ry), columns_of(in_ref, ry + 1)
        kept = jnp.concatenate(
            [in_ref[:, ry + k, 32:48, :].reshape(HALF, 128) for k in range(2)], axis=1
        ).astype(F32) > 0
        parts = []
        for p in range(2):
            first = jnp.concatenate([a[p], b[p]], axis=1).astype(F32)
            parts.append(jnp.where(kept, first, z[p * HALF : (p + 1) * HALF]).astype(BF16))
        forward_columns(jnp.concatenate(parts, axis=0), fx_ref, tw_ref, v_ref, ry)
    put_largest(forward_tiles(v_ref, wf_ref, c2_ref), top_ref)


def last_kernel(level_ref, c_ref, tops_ref, ix_ref, tw_ref, wi_ref, out_ref, o_ref):
    shrink_tiles(c_ref, tops_ref, level_ref[1], wi_ref, o_ref)
    for ry in range(0, TILES, 2):
        z = inverse_columns(o_ref, ix_ref, tw_ref, ry).astype(BF16)
        for k in range(2):
            for p in range(2):
                part = z[p * HALF : (p + 1) * HALF, k * 128 : (k + 1) * 128]
                out_ref[:, ry + k, p * 16 : (p + 1) * 16, :] = part.reshape(NRX, 16, 128)


COEFFS = jax.ShapeDtypeStruct((TILES, HALF, 384), F32)
TOPS = jax.ShapeDtypeStruct((NF, 1, 128), F32)
V_SCRATCH = pltpu.VMEM((2, HALF, TILES * 128), BF16)
O_SCRATCH = pltpu.VMEM((TILES, HALF, 512), F32)
SMEM = pl.BlockSpec(memory_space=pltpu.SMEM)
VMEM = pl.BlockSpec(memory_space=pltpu.VMEM)


def first_half(arrived, fx, tw, wf):
    return pl.pallas_call(
        first_kernel,
        in_specs=[VMEM] * 4,
        out_specs=[VMEM] * 2,
        out_shape=[COEFFS, TOPS],
        scratch_shapes=[V_SCRATCH],
        name="first",
    )(arrived, fx, tw, wf)


def middle(levels, c, tops, arrived, fx, ix, tw, wf, wi):
    return pl.pallas_call(
        middle_kernel,
        in_specs=[SMEM] + [VMEM] * 8,
        out_specs=[VMEM] * 2,
        out_shape=[COEFFS, TOPS],
        scratch_shapes=[O_SCRATCH, V_SCRATCH],
        name="middle",
    )(levels, c, tops, arrived, fx, ix, tw, wf, wi)


def last_half(levels, c, tops, ix, tw, wi):
    return pl.pallas_call(
        last_kernel,
        in_specs=[SMEM] + [VMEM] * 5,
        out_specs=VMEM,
        out_shape=jax.ShapeDtypeStruct((NRX, TILES, 32, 128), BF16),
        scratch_shapes=[O_SCRATCH],
        name="last",
    )(levels, c, tops, ix, tw, wi)


def rebuild_kernel(in_ref, record_ref, mask_ref, table_ref, out_ref, hold_ref):
    step = pl.program_id(0)

    @pl.when(step == 0)
    def _():
        for f in range(NF):
            hold_ref[f * PAD3 : f * PAD3 + 32, :] = in_ref[f].astype(F32)

    blocks = record_ref.shape[0] // 2
    for b in range(blocks):
        row = step * blocks + b
        spec = jnp.concatenate(
            [hold_ref[pl.ds(p * 16 + row, NF, stride=PAD3), :] for p in range(2)], axis=0
        )
        spec = (spec * (2.0 / NT)).astype(BF16)
        recon = lax.dot_general(
            spec, table_ref[...], (((0,), (0,)), ((), ())), preferred_element_type=F32
        )
        kept = jnp.transpose(jnp.broadcast_to(mask_ref[pl.ds(row, 1), :], (128, 128)))
        rec = record_ref[2 * b : 2 * b + 2].reshape(128, NT).astype(F32)
        for t in range(0, NT, 128):
            mixed = jnp.where(kept > 0, rec[:, t : t + 128], recon[:, t : t + 128])
            out_ref[2 * b : 2 * b + 2, :, t : t + 128] = mixed.astype(BF16).reshape(2, CY, 128)


def rebuild(returned, record, flags, table):
    rows = 4
    return pl.pallas_call(
        rebuild_kernel,
        grid=(CX // rows,),
        in_specs=[
            pl.BlockSpec((NF, 32, 128), lambda i: (0, 0, 0)),
            pl.BlockSpec((rows, CY, NT), lambda i: (i, 0, 0)),
            pl.BlockSpec((16, 128), lambda i: (0, 0)),
            pl.BlockSpec((2 * NF, NT), lambda i: (0, 0)),
        ],
        out_specs=pl.BlockSpec((rows, CY, NT), lambda i: (i, 0, 0)),
        out_shape=jax.ShapeDtypeStruct((CX, CY, NT), BF16),
        scratch_shapes=[pltpu.VMEM((NF * PAD3, 128), F32)],
        name="rebuild",
    )(returned, record, flags, table)


def exchange(array):
    return lax.all_to_all(array, ALL, split_axis=0, concat_axis=0, tiled=True)


def tables():
    fx, ix = plane_tables()
    wf, wi = window_tables()
    narrow = [np.asarray(t, jnp.bfloat16) for t in (time_table(), fx, ix, wf, wi)]
    return (*narrow, np.asarray(twiddle_table(), np.float32))


def body(record, sampled, levels):
    time, fx, ix, wf, wi, tw = tables()
    flags = sampled.astype(F32).reshape(16, 128)
    sent = spectra_of(record, flags, time)
    arrived = exchange(sent).reshape(NRX, TILES, 48, 128)
    c, top = first_half(arrived, fx, tw, wf)
    c, top = middle(levels, c, exchange(top), arrived, fx, ix, tw, wf, wi)
    back = last_half(levels, c, exchange(top), ix, tw, wi)
    returned = exchange(back.reshape(NF, 32, 128))
    return rebuild(returned, record, flags, time)


def solution(mesh):
    finer = Mesh(mesh.devices.reshape(2, 4, 2, 2, 4), ALL)
    rx, ry = ALL[:3], ALL[3:]
    return jax.shard_map(
        body,
        mesh=finer,
        in_specs=(P(rx, ry, None), P(rx, ry), P()),
        out_specs=P(rx, ry, None),
        check_vma=False,
    )
```

```python
import functools

import jax
import jax.numpy as jnp
import numpy as np
from jax import lax
from jax.experimental import pallas as pl
from jax.experimental.pallas import tpu as pltpu
from jax.sharding import Mesh
from jax.sharding import PartitionSpec as P

H = 16
NF = 128
FLO = 8
CX, CY, NT = 32, 64, 2048
LX = 512
HALF = LX // 2
TILES = 8
WIN = CY + 2 * H
NRX = LX // CX
ALL = ("rx_0", "rx_1", "rx_2", "ry_0", "ry_1")
F32 = jnp.float32
BF16 = jnp.bfloat16
PAD = 264
PAD3 = 40
SMEM = pl.BlockSpec(memory_space=pltpu.SMEM)
VMEM = pl.BlockSpec(memory_space=pltpu.VMEM)


def time_table():
    f = FLO + np.arange(NF)[:, None]
    ang = 2.0 * np.pi * (f * np.arange(NT)[None, :] % NT) / NT
    return np.concatenate([np.cos(ang), -np.sin(ang)], axis=0)


def plane_tables():
    n = np.arange(HALF)
    ang = 2.0 * np.pi * (n[:, None] * n[None, :] % HALF) / HALF
    c, s = np.cos(ang), np.sin(ang)
    forward = np.block([[c, s], [-s, c]])
    inverse = np.block([[c, -s], [s, c]]) / LX
    return forward, inverse


def twiddle_table():
    ang = 2.0 * np.pi * np.arange(HALF)[:, None] / LX
    ones = np.ones((HALF, CY))
    real = np.concatenate([ones, np.cos(ang) * ones], axis=1)
    imag = np.concatenate([0.0 * ones, -np.sin(ang) * ones], axis=1)
    return np.concatenate([real, imag], axis=0)


def taper():
    s = np.arange(WIN)
    rising = np.sin(0.5 * np.pi * (s + 0.5) / (2 * H))
    falling = np.cos(0.5 * np.pi * (s - CY + 0.5) / (2 * H))
    return np.where(s < 2 * H, rising, np.where(s >= CY, falling, 1.0))


def window_tables():
    k = np.arange(WIN)
    ang = 2.0 * np.pi * (k[:, None] * k[None, :] % WIN) / WIN
    w = taper()
    ya, yb = w[None, :] * np.cos(ang), w[None, :] * np.sin(ang)
    yc, yd = w[:, None] / WIN * np.cos(ang), w[:, None] / WIN * np.sin(ang)
    fwd = np.zeros((256, 256))
    inv = np.zeros((256, 256))
    for y in range(CY):
        spots = [(y, y + H)]
        if y < H:
            spots.append((128 + y, CY + H + y))
        if y >= CY - H:
            spots.append((128 + y, y - (CY - H)))
        for re, s in spots:
            im = re + CY
            fwd[re, :WIN] = ya[:, s]
            fwd[im, :WIN] = yb[:, s]
            fwd[im, 128 : 128 + WIN] = ya[:, s]
            fwd[re, 128 : 128 + WIN] = -yb[:, s]
            inv[:WIN, re] = yc[s, :]
            inv[128 : 128 + WIN, re] = -yd[s, :]
            inv[128 : 128 + WIN, im] = yc[s, :]
            inv[:WIN, im] = yd[s, :]
    return fwd, inv


MIB = 1024 * 1024
ROWS = 40


def limit(mib):
    return pltpu.CompilerParams(vmem_limit_bytes=int(mib * MIB))


def lane_flags(mask_ref):
    even = mask_ref[pl.ds(0, 16, stride=2), :]
    odd = mask_ref[pl.ds(1, 16, stride=2), :]
    return jnp.concatenate([even, odd], axis=1).astype(F32)


def spectra_kernel(
    record_ref, mask_ref, table_hbm, out_ref, in_ref, table_ref, hold_ref, flag_ref, sems, table_sem
):
    chunk, ahead = 8, 2
    chunks = CX // chunk

    def copy(i):
        part = pl.ds(i * chunk, chunk)
        return pltpu.make_async_copy(record_ref.at[part], in_ref.at[part], sems.at[i])

    table_copy = pltpu.make_async_copy(table_hbm, table_ref, table_sem)
    table_copy.start()
    for i in range(ahead):
        copy(i).start()
    flag_ref[...] = lane_flags(mask_ref)
    table_copy.wait()

    def transform(i, carry):
        copy(i).wait()

        @pl.when(i + ahead < chunks)
        def _():
            copy(i + ahead).start()

        traces = in_ref[pl.ds(i * chunk, chunk)].reshape(-1, NT)
        res = lax.dot_general(
            table_ref[...], traces, (((1,), (1,)), ((), ())), preferred_element_type=F32
        )
        for b in range(chunk // 2):
            row = i * (chunk // 2) + b
            kept = flag_ref[pl.ds(row, 1), :]
            value = jnp.where(kept > 0, res[:, b * 128 : (b + 1) * 128], 0.0)
            hold_ref[pl.ds(pl.multiple_of(row * PAD, 8), 2 * NF), :] = value
        return carry

    lax.fori_loop(0, chunks, transform, 0)
    halves = [flag_ref[c * 8 : (c + 1) * 8, :].astype(BF16) for c in range(2)]

    def place(group, carry):
        for k in range(16):
            f = group * 16 + k
            for p in range(2):
                part = hold_ref[pl.ds(p * NF + f, 16, stride=PAD), :]
                out_ref[f, p * 16 : (p + 1) * 16, :] = part.astype(BF16)
            out_ref[f, 32:40, :] = halves[k // 8]
        return carry

    lax.fori_loop(0, NF // 16, place, 0)


def spectra_of(record, sampled, table):
    hbm = pl.BlockSpec(memory_space=pltpu.HBM)
    return pl.pallas_call(
        spectra_kernel,
        in_specs=[hbm, VMEM, hbm],
        out_specs=VMEM,
        out_shape=jax.ShapeDtypeStruct((NF, ROWS, 128), BF16),
        scratch_shapes=[
            pltpu.VMEM((CX, CY, NT), BF16),
            pltpu.VMEM((2 * NF, NT), BF16),
            pltpu.VMEM((16 * PAD, 128), F32),
            pltpu.VMEM((16, 128), F32),
            pltpu.SemaphoreType.DMA((CX // 8,)),
            pltpu.SemaphoreType.DMA,
        ],
        compiler_params=limit(51),
        name="spectra",
    )(record, sampled, table)


GROUP = 4


def early_lanes(rows):
    return lax.broadcasted_iota(jnp.int32, (rows, 128), 1) % CY < CY // 2


def low_lanes():
    return lax.broadcasted_iota(jnp.int32, (HALF, 128), 1) < CY


def side_by_side(blocks):
    return jnp.concatenate(blocks, axis=1)


def columns_of(in_ref, ry, p):
    return in_ref[:, ry, p * 16 : (p + 1) * 16, :].reshape(HALF, 128)


def forward_columns(data, fx_ref, tw_ref, v_ref, start):
    res = jnp.dot(fx_ref[...], data, preferred_element_type=F32)
    tr, ti = tw_ref[:HALF], tw_ref[HALF:]
    low = low_lanes()
    for k in range(GROUP):
        at = k * 128
        ar, ai = res[:HALF, at : at + 128], res[HALF:, at : at + 128]
        br = ar * tr - ai * ti
        bi = ar * ti + ai * tr
        first = jnp.where(low, br, pltpu.roll(bi, CY, 1))
        second = jnp.where(low, pltpu.roll(br, CY, 1), bi)
        v_ref[start + k, :HALF] = (first + second).astype(BF16)
        v_ref[start + k, HALF:] = (first - second).astype(BF16)


def forward_tiles(v_ref, wf_ref, c_ref):
    early = early_lanes(LX)
    best = jnp.zeros((8, 128), F32)
    for j in range(TILES):
        left, right = (j + TILES - 1) % TILES, (j + 1) % TILES
        near = jnp.where(early, v_ref[right], v_ref[left])
        c = jnp.dot(side_by_side([v_ref[j], near]), wf_ref[...], preferred_element_type=F32)
        c_ref[j] = c
        squares = c[:, :128] * c[:, :128] + c[:, 128:] * c[:, 128:]
        best = jnp.maximum(best, jnp.max(squares.reshape(-1, 8, 128), axis=0))
    return best


def put_largest(best, top_ref):
    top = jnp.sqrt(jnp.max(best, keepdims=True))
    top_ref[...] = jnp.broadcast_to(top.reshape(1, 1, 1), top_ref.shape)


def shrink_tiles(c_ref, tops_ref, level, wi_ref, o_ref):
    tau = level.astype(F32) * 0.001 * (jnp.max(tops_ref[...]) + 1e-06)
    for j in range(TILES):
        real, imag = c_ref[j, :, :128], c_ref[j, :, 128:]
        g = jnp.maximum(1.0 - tau * lax.rsqrt(real * real + imag * imag), 0.0)
        e = side_by_side([real * g, imag * g]).astype(BF16)
        o_ref[j] = jnp.dot(e, wi_ref[...], preferred_element_type=F32)


def inverse_columns(o_ref, ix_ref, tw_ref, start):
    tr, ti = tw_ref[:HALF], tw_ref[HALF:]
    low, early = low_lanes(), early_lanes(LX)
    reals, imags = [], []
    for j in range(start, start + GROUP):
        left, right = (j + TILES - 1) % TILES, (j + 1) % TILES
        near = jnp.where(early, o_ref[left, :, 128:], o_ref[right, :, 128:])
        both = o_ref[j, :, :128] + near
        total, apart = both[:HALF] + both[HALF:], both[:HALF] - both[HALF:]
        real = jnp.where(low, total, pltpu.roll(apart, CY, 1))
        imag = jnp.where(low, pltpu.roll(total, CY, 1), apart)
        reals.append((real * tr + imag * ti).astype(BF16))
        imags.append((imag * tr - real * ti).astype(BF16))
    g = jnp.concatenate([side_by_side(reals), side_by_side(imags)], axis=0)
    return jnp.dot(ix_ref[...], g, preferred_element_type=F32)


def first_kernel(in_ref, fx_ref, tw_ref, wf_ref, c_ref, top_ref, v_ref):
    for start in range(0, TILES, GROUP):
        parts = [
            side_by_side([columns_of(in_ref, start + k, p) for k in range(GROUP)])
            for p in range(2)
        ]
        forward_columns(jnp.concatenate(parts, axis=0), fx_ref, tw_ref, v_ref, start)
    put_largest(forward_tiles(v_ref, wf_ref, c_ref), top_ref)


def middle_kernel(
    level_ref, core_ref, c_ref, tops_ref, in_ref, flag_ref, fx_ref, ix_ref, tw_ref, wf_ref, wi_ref,
    c2_ref, top_ref, o_ref, v_ref,
):
    shrink_tiles(c_ref, tops_ref, level_ref[0], wi_ref, o_ref)
    on_first = core_ref[0] == 0
    for start in range(0, TILES, GROUP):
        z = inverse_columns(o_ref, ix_ref, tw_ref, start)
        kept = []
        for k in range(GROUP):
            mine = in_ref[:, start + k, 32:40, :].astype(F32)
            other = flag_ref[:, start + k].astype(F32)
            upper, lower = jnp.where(on_first, mine, other), jnp.where(on_first, other, mine)
            kept.append(jnp.concatenate([upper, lower], axis=1).reshape(HALF, 128))
        kept = side_by_side(kept) > 0
        parts = []
        for p in range(2):
            sent = side_by_side([columns_of(in_ref, start + k, p) for k in range(GROUP)])
            fresh = z[p * HALF : (p + 1) * HALF]
            parts.append(jnp.where(kept, sent.astype(F32), fresh).astype(BF16))
        forward_columns(jnp.concatenate(parts, axis=0), fx_ref, tw_ref, v_ref, start)
    put_largest(forward_tiles(v_ref, wf_ref, c2_ref), top_ref)


def last_kernel(level_ref, c_ref, tops_ref, ix_ref, tw_ref, wi_ref, out_ref, o_ref):
    shrink_tiles(c_ref, tops_ref, level_ref[1], wi_ref, o_ref)
    for start in range(0, TILES, GROUP):
        z = inverse_columns(o_ref, ix_ref, tw_ref, start).astype(BF16)
        for k in range(GROUP):
            for p in range(2):
                part = z[p * HALF : (p + 1) * HALF, k * 128 : (k + 1) * 128]
                out_ref[:, start + k, p * 16 : (p + 1) * 16, :] = part.reshape(NRX, 16, 128)


COEFFS = jax.ShapeDtypeStruct((TILES, LX, 256), F32)
TOPS = jax.ShapeDtypeStruct((NF, 1, 128), F32)
V_SCRATCH = pltpu.VMEM((TILES, LX, 128), BF16)
O_SCRATCH = pltpu.VMEM((TILES, LX, 256), F32)


def first_half(arrived, fx, tw, wf):
    return pl.pallas_call(
        first_kernel,
        in_specs=[VMEM] * 4,
        out_specs=[VMEM] * 2,
        out_shape=[COEFFS, TOPS],
        scratch_shapes=[V_SCRATCH],
        compiler_params=limit(18),
        name="first",
    )(arrived, fx, tw, wf)


def middle(levels, core, c, tops, arrived, flags, fx, ix, tw, wf, wi):
    return pl.pallas_call(
        middle_kernel,
        in_specs=[SMEM] * 2 + [VMEM] * 9,
        out_specs=[VMEM] * 2,
        out_shape=[COEFFS, TOPS],
        scratch_shapes=[O_SCRATCH, V_SCRATCH],
        compiler_params=limit(26),
        name="middle",
    )(levels, core, c, tops, arrived, flags, fx, ix, tw, wf, wi)


def last_half(levels, c, tops, ix, tw, wi):
    return pl.pallas_call(
        last_kernel,
        in_specs=[SMEM] + [VMEM] * 5,
        out_specs=VMEM,
        out_shape=jax.ShapeDtypeStruct((NRX, TILES, 32, 128), BF16),
        scratch_shapes=[O_SCRATCH],
        compiler_params=limit(18),
        name="last",
    )(levels, c, tops, ix, tw, wi)


CHUNK = 4
CHUNKS = CX // CHUNK


def rebuild_kernel(in_ref, record_ref, mask_ref, table_ref, out_ref, made_ref, hold_ref, sems):
    def spread(group, carry):
        for k in range(8):
            f = group * 8 + k
            at = pl.ds(pl.multiple_of(f * PAD3, 8), 32)
            hold_ref[at, :] = in_ref[f].astype(F32) * (2.0 / NT)
        return carry

    lax.fori_loop(0, NF // 8, spread, 0)
    flags = lane_flags(mask_ref)

    def copy(i):
        part = pl.ds(i * CHUNK, CHUNK)
        return pltpu.make_async_copy(made_ref.at[part], out_ref.at[part], sems.at[i])

    for i in range(CHUNKS):
        for x in range(i * CHUNK, (i + 1) * CHUNK, 2):
            row = x // 2
            spec = jnp.concatenate(
                [hold_ref[pl.ds(p * 16 + row, NF, stride=PAD3), :] for p in range(2)], axis=0
            ).astype(BF16)
            recon = lax.dot_general(
                spec, table_ref[...], (((0,), (0,)), ((), ())), preferred_element_type=F32
            )
            kept = jnp.transpose(jnp.broadcast_to(flags[row : row + 1], (128, 128))) > 0
            rec = record_ref[x : x + 2].reshape(128, NT).astype(F32)
            for t in range(0, NT, 128):
                mixed = jnp.where(kept, rec[:, t : t + 128], recon[:, t : t + 128])
                made_ref[x : x + 2, :, t : t + 128] = mixed.astype(BF16).reshape(2, CY, 128)
        copy(i).start()
    for i in range(CHUNKS):
        copy(i).wait()


def rebuild(returned, record, sampled, table):
    return pl.pallas_call(
        rebuild_kernel,
        in_specs=[VMEM] * 4,
        out_specs=pl.BlockSpec(memory_space=pltpu.HBM),
        out_shape=jax.ShapeDtypeStruct((CX, CY, NT), BF16),
        scratch_shapes=[
            pltpu.VMEM((CX, CY, NT), BF16),
            pltpu.VMEM((NF * PAD3, 128), F32),
            pltpu.SemaphoreType.DMA((CHUNKS,)),
        ],
        compiler_params=limit(26),
        name="rebuild",
    )(returned, record, sampled, table)


def exchange(array):
    return lax.all_to_all(array, ALL, split_axis=0, concat_axis=0, tiled=True)


def tables():
    fx, ix = plane_tables()
    wf, wi = window_tables()
    narrow = [np.asarray(t, jnp.bfloat16) for t in (time_table(), fx, ix, wf, wi)]
    return (*narrow, np.asarray(twiddle_table(), np.float32))


def body(record, sampled, levels):
    time, fx, ix, wf, wi, tw = tables()
    sent = spectra_of(record, sampled, time)
    arrived = exchange(sent).reshape(NRX, TILES, ROWS, 128)
    flags = lax.ppermute(arrived[:, :, 32:40, :], ALL[2], [(0, 1), (1, 0)])
    c, top = first_half(arrived, fx, tw, wf)
    core = lax.axis_index(ALL[2]).reshape(1)
    top, flags, core = lax.optimization_barrier((top, flags, core))
    c, top = middle(levels, core, c, exchange(top), arrived, flags, fx, ix, tw, wf, wi)
    back = last_half(levels, c, exchange(top), ix, tw, wi)
    returned = exchange(back.reshape(NF, 32, 128))
    return rebuild(returned, record, sampled, time)


def solution(mesh):
    finer = Mesh(mesh.devices.reshape(2, 4, 2, 2, 4), ALL)
    rx, ry = ALL[:3], ALL[3:]
    return jax.shard_map(
        body,
        mesh=finer,
        in_specs=(P(rx, ry, None), P(rx, ry), P()),
        out_specs=P(rx, ry, None),
        check_vma=False,
    )
```

```python
import functools

import jax
import jax.numpy as jnp
import numpy as np
from jax import lax
from jax.experimental import pallas as pl
from jax.experimental.pallas import tpu as pltpu
from jax.sharding import Mesh
from jax.sharding import PartitionSpec as P

H = 16
NF = 128
FLO = 8
CX, CY, NT = 32, 64, 2048
LX = 512
HALF = LX // 2
QUARTER = LX // 4
TILES = 8
WIN = CY + 2 * H
NRX = LX // CX
ALL = ("rx_0", "rx_1", "rx_2", "ry_0", "ry_1")
F32 = jnp.float32
BF16 = jnp.bfloat16
PAD = 264
PAD3 = 40
SMEM = pl.BlockSpec(memory_space=pltpu.SMEM)
VMEM = pl.BlockSpec(memory_space=pltpu.VMEM)


def time_table():
    f = FLO + np.arange(NF)[:, None]
    ang = 2.0 * np.pi * (f * np.arange(NT)[None, :] % NT) / NT
    return np.concatenate([np.cos(ang), -np.sin(ang)], axis=0)


def plane_tables():
    a, m = np.arange(QUARTER)[None, :], np.arange(QUARTER)[:, None]
    blocks = []
    for odd in range(2):
        ang = 2.0 * np.pi * (a * (2 * m + odd) % HALF) / HALF
        c, s = np.cos(ang), np.sin(ang)
        blocks.append(np.block([[c, s], [-s, c]]))
    return np.concatenate(blocks), np.concatenate([b.T for b in blocks]) / LX


def twiddle_table():
    order = np.concatenate([np.arange(0, HALF, 2), np.arange(1, HALF, 2)])
    ang = 2.0 * np.pi * order[:, None] / LX
    ones = np.ones((HALF, CY))
    real = np.concatenate([ones, np.cos(ang) * ones], axis=1)
    imag = np.concatenate([0.0 * ones, -np.sin(ang) * ones], axis=1)
    return np.concatenate([real, imag], axis=0)


def taper():
    s = np.arange(WIN)
    rising = np.sin(0.5 * np.pi * (s + 0.5) / (2 * H))
    falling = np.cos(0.5 * np.pi * (s - CY + 0.5) / (2 * H))
    return np.where(s < 2 * H, rising, np.where(s >= CY, falling, 1.0))


def window_tables():
    k = np.arange(WIN)
    ang = 2.0 * np.pi * (k[:, None] * k[None, :] % WIN) / WIN
    w = taper()
    ya, yb = w[None, :] * np.cos(ang), w[None, :] * np.sin(ang)
    yc, yd = w[:, None] / WIN * np.cos(ang), w[:, None] / WIN * np.sin(ang)
    fwd = np.zeros((256, 256))
    inv = np.zeros((256, 256))
    for y in range(CY):
        spots = [(y, y + H)]
        if y < H:
            spots.append((128 + y, CY + H + y))
        if y >= CY - H:
            spots.append((128 + y, y - (CY - H)))
        for re, s in spots:
            im = re + CY
            fwd[re, :WIN] = ya[:, s]
            fwd[im, :WIN] = yb[:, s]
            fwd[im, 128 : 128 + WIN] = ya[:, s]
            fwd[re, 128 : 128 + WIN] = -yb[:, s]
            inv[:WIN, re] = yc[s, :]
            inv[128 : 128 + WIN, re] = -yd[s, :]
            inv[128 : 128 + WIN, im] = yc[s, :]
            inv[:WIN, im] = yd[s, :]
    return fwd, inv


MIB = 1024 * 1024
ROWS = 40


def limit(mib):
    return pltpu.CompilerParams(vmem_limit_bytes=int(mib * MIB))


def lane_flags(mask_ref):
    even = mask_ref[pl.ds(0, 16, stride=2), :]
    odd = mask_ref[pl.ds(1, 16, stride=2), :]
    return jnp.concatenate([even, odd], axis=1).astype(F32)


def make_time_table(table_ref):
    f = FLO + lax.broadcasted_iota(jnp.int32, (NF, 128), 0)
    n = lax.broadcasted_iota(jnp.int32, (NF, 128), 1)
    fine = (f * n % NT).astype(F32) * (2.0 * np.pi / NT)
    coarse = (f * n % (NT // 128)).astype(F32) * (2.0 * np.pi * 128 / NT)
    cos_fine, sin_fine = jnp.cos(fine), jnp.sin(fine)
    cos_coarse, sin_coarse = jnp.cos(coarse), jnp.sin(coarse)
    for u in range(NT // 128):
        c, s = cos_coarse[:, u : u + 1], sin_coarse[:, u : u + 1]
        at = u * 128
        table_ref[:NF, at : at + 128] = (c * cos_fine - s * sin_fine).astype(BF16)
        table_ref[NF:, at : at + 128] = (-(s * cos_fine + c * sin_fine)).astype(BF16)


def spectra_kernel(record_ref, mask_ref, out_ref, in_ref, table_ref, hold_ref, flag_ref, sems):
    chunk, ahead = 8, 3
    chunks = CX // chunk

    def copy(i):
        part = pl.ds(i * chunk, chunk)
        return pltpu.make_async_copy(record_ref.at[part], in_ref.at[part], sems.at[i])

    for i in range(ahead):
        copy(i).start()
    flag_ref[...] = lane_flags(mask_ref)
    make_time_table(table_ref)

    def transform(i, carry):
        copy(i).wait()

        @pl.when(i + ahead < chunks)
        def _():
            copy(i + ahead).start()

        traces = in_ref[pl.ds(i * chunk, chunk)].reshape(-1, NT)
        res = lax.dot_general(
            table_ref[...], traces, (((1,), (1,)), ((), ())), preferred_element_type=F32
        )
        for b in range(chunk // 2):
            row = i * (chunk // 2) + b
            kept = flag_ref[pl.ds(row, 1), :]
            value = jnp.where(kept > 0, res[:, b * 128 : (b + 1) * 128], 0.0)
            hold_ref[pl.ds(pl.multiple_of(row * PAD, 8), 2 * NF), :] = value
        return carry

    lax.fori_loop(0, chunks, transform, 0)
    halves = [flag_ref[c * 8 : (c + 1) * 8, :].astype(BF16) for c in range(2)]

    def place(group, carry):
        for k in range(16):
            f = group * 16 + k
            for p in range(2):
                part = hold_ref[pl.ds(p * NF + f, 16, stride=PAD), :]
                out_ref[f, p * 16 : (p + 1) * 16, :] = part.astype(BF16)
            out_ref[f, 32:40, :] = halves[k // 8]
        return carry

    lax.fori_loop(0, NF // 16, place, 0)


def spectra_of(record, sampled):
    return pl.pallas_call(
        spectra_kernel,
        in_specs=[pl.BlockSpec(memory_space=pltpu.HBM), VMEM],
        out_specs=VMEM,
        out_shape=jax.ShapeDtypeStruct((NF, ROWS, 128), BF16),
        scratch_shapes=[
            pltpu.VMEM((CX, CY, NT), BF16),
            pltpu.VMEM((2 * NF, NT), BF16),
            pltpu.VMEM((16 * PAD, 128), F32),
            pltpu.VMEM((16, 128), F32),
            pltpu.SemaphoreType.DMA((CX // 8,)),
        ],
        compiler_params=limit(51),
        name="spectra",
    )(record, sampled)


GROUP = 4


def early_lanes(rows):
    return lax.broadcasted_iota(jnp.int32, (rows, 128), 1) % CY < CY // 2


def low_lanes():
    return lax.broadcasted_iota(jnp.int32, (QUARTER, 128), 1) < CY


def side_by_side(blocks):
    return jnp.concatenate(blocks, axis=1)


def columns_of(in_ref, ry, p):
    return in_ref[:, ry, p * 16 : (p + 1) * 16, :].reshape(HALF, 128)


def forward_columns(parts, fx_ref, tw_ref, v_ref, start):
    low = low_lanes()
    for odd in range(2):
        upper, lower = [x[:QUARTER] for x in parts], [x[QUARTER:] for x in parts]
        data = jnp.concatenate([u - w if odd else u + w for u, w in zip(upper, lower)], axis=0)
        table = fx_ref[odd * HALF : (odd + 1) * HALF]
        res = jnp.dot(table, data, preferred_element_type=F32)
        rows = odd * QUARTER
        tr = tw_ref[rows : rows + QUARTER]
        ti = tw_ref[HALF + rows : HALF + rows + QUARTER]
        for k in range(GROUP):
            at = k * 128
            ar, ai = res[:QUARTER, at : at + 128], res[QUARTER:, at : at + 128]
            br = ar * tr - ai * ti
            bi = ar * ti + ai * tr
            first = jnp.where(low, br, pltpu.roll(bi, CY, 1))
            second = jnp.where(low, pltpu.roll(br, CY, 1), bi)
            v_ref[start + k, rows : rows + QUARTER] = (first + second).astype(BF16)
            v_ref[start + k, HALF + rows : HALF + rows + QUARTER] = (first - second).astype(BF16)


def forward_tiles(v_ref, wf_ref, c_ref):
    early = early_lanes(LX)
    best = jnp.zeros((8, 128), F32)
    for j in range(TILES):
        left, right = (j + TILES - 1) % TILES, (j + 1) % TILES
        near = jnp.where(early, v_ref[right], v_ref[left])
        c = jnp.dot(side_by_side([v_ref[j], near]), wf_ref[...], preferred_element_type=F32)
        c_ref[j] = c
        squares = c[:, :128] * c[:, :128] + c[:, 128:] * c[:, 128:]
        best = jnp.maximum(best, jnp.max(squares.reshape(-1, 8, 128), axis=0))
    return best


def put_largest(best, top_ref):
    top = jnp.sqrt(jnp.max(best, keepdims=True))
    top_ref[...] = jnp.broadcast_to(top.reshape(1, 1, 1), top_ref.shape)


def shrink_tiles(c_ref, tops_ref, level, wi_ref, o_ref):
    tau = level.astype(F32) * 0.001 * (jnp.max(tops_ref[...]) + 1e-06)
    for j in range(TILES):
        real, imag = c_ref[j, :, :128], c_ref[j, :, 128:]
        g = jnp.maximum(1.0 - tau * lax.rsqrt(real * real + imag * imag), 0.0)
        e = side_by_side([real * g, imag * g]).astype(BF16)
        o_ref[j] = jnp.dot(e, wi_ref[...], preferred_element_type=F32)


def inverse_columns(o_ref, ix_ref, tw_ref, start):
    low, early = low_lanes(), early_lanes(QUARTER)
    made = []
    for odd in range(2):
        rows = odd * QUARTER
        tr = tw_ref[rows : rows + QUARTER]
        ti = tw_ref[HALF + rows : HALF + rows + QUARTER]
        reals, imags = [], []
        for j in range(start, start + GROUP):
            left, right = (j + TILES - 1) % TILES, (j + 1) % TILES
            halves = []
            for at in (rows, HALF + rows):
                part = pl.ds(at, QUARTER)
                near = jnp.where(early, o_ref[left, part, 128:], o_ref[right, part, 128:])
                halves.append(o_ref[j, part, :128] + near)
            total, apart = halves[0] + halves[1], halves[0] - halves[1]
            real = jnp.where(low, total, pltpu.roll(apart, CY, 1))
            imag = jnp.where(low, pltpu.roll(total, CY, 1), apart)
            reals.append((real * tr + imag * ti).astype(BF16))
            imags.append((imag * tr - real * ti).astype(BF16))
        g = jnp.concatenate([side_by_side(reals), side_by_side(imags)], axis=0)
        table = ix_ref[odd * HALF : (odd + 1) * HALF]
        made.append(jnp.dot(table, g, preferred_element_type=F32))
    even, odd = made
    return [
        jnp.concatenate([even[at : at + QUARTER] + odd[at : at + QUARTER],
                         even[at : at + QUARTER] - odd[at : at + QUARTER]], axis=0).astype(BF16)
        for at in (0, QUARTER)
    ]


def first_kernel(in_ref, fx_ref, tw_ref, wf_ref, c_ref, top_ref, v_ref):
    for start in range(0, TILES, GROUP):
        parts = [
            side_by_side([columns_of(in_ref, start + k, p) for k in range(GROUP)])
            for p in range(2)
        ]
        forward_columns(parts, fx_ref, tw_ref, v_ref, start)
    put_largest(forward_tiles(v_ref, wf_ref, c_ref), top_ref)


def middle_kernel(
    level_ref, core_ref, c_ref, tops_ref, in_ref, flag_ref, fx_ref, ix_ref, tw_ref, wf_ref, wi_ref,
    c2_ref, top_ref, o_ref, v_ref,
):
    shrink_tiles(c_ref, tops_ref, level_ref[0], wi_ref, o_ref)
    on_first = core_ref[0] == 0
    for start in range(0, TILES, GROUP):
        fresh = inverse_columns(o_ref, ix_ref, tw_ref, start)
        kept = []
        for k in range(GROUP):
            mine = in_ref[:, start + k, 32:40, :].astype(F32)
            other = flag_ref[:, start + k].astype(F32)
            upper, lower = jnp.where(on_first, mine, other), jnp.where(on_first, other, mine)
            kept.append(jnp.concatenate([upper, lower], axis=1).reshape(HALF, 128))
        kept = side_by_side(kept) > 0
        parts = []
        for p in range(2):
            sent = side_by_side([columns_of(in_ref, start + k, p) for k in range(GROUP)])
            parts.append(jnp.where(kept, sent, fresh[p]))
        forward_columns(parts, fx_ref, tw_ref, v_ref, start)
    put_largest(forward_tiles(v_ref, wf_ref, c2_ref), top_ref)


def last_kernel(level_ref, c_ref, tops_ref, ix_ref, tw_ref, wi_ref, out_ref, o_ref):
    shrink_tiles(c_ref, tops_ref, level_ref[1], wi_ref, o_ref)
    for start in range(0, TILES, GROUP):
        fresh = inverse_columns(o_ref, ix_ref, tw_ref, start)
        for k in range(GROUP):
            for p in range(2):
                part = fresh[p][:, k * 128 : (k + 1) * 128]
                out_ref[:, start + k, p * 16 : (p + 1) * 16, :] = part.reshape(NRX, 16, 128)


COEFFS = jax.ShapeDtypeStruct((TILES, LX, 256), F32)
TOPS = jax.ShapeDtypeStruct((NF, 1, 128), F32)
V_SCRATCH = pltpu.VMEM((TILES, LX, 128), BF16)
O_SCRATCH = pltpu.VMEM((TILES, LX, 256), F32)


def first_half(arrived, fx, tw, wf):
    return pl.pallas_call(
        first_kernel,
        in_specs=[VMEM] * 4,
        out_specs=[VMEM] * 2,
        out_shape=[COEFFS, TOPS],
        scratch_shapes=[V_SCRATCH],
        compiler_params=limit(18),
        name="first",
    )(arrived, fx, tw, wf)


def middle(levels, core, c, tops, arrived, flags, fx, ix, tw, wf, wi):
    return pl.pallas_call(
        middle_kernel,
        in_specs=[SMEM] * 2 + [VMEM] * 9,
        out_specs=[VMEM] * 2,
        out_shape=[COEFFS, TOPS],
        scratch_shapes=[O_SCRATCH, V_SCRATCH],
        compiler_params=limit(26),
        name="middle",
    )(levels, core, c, tops, arrived, flags, fx, ix, tw, wf, wi)


def last_half(levels, c, tops, ix, tw, wi):
    return pl.pallas_call(
        last_kernel,
        in_specs=[SMEM] + [VMEM] * 5,
        out_specs=VMEM,
        out_shape=jax.ShapeDtypeStruct((NRX, TILES, 32, 128), BF16),
        scratch_shapes=[O_SCRATCH],
        compiler_params=limit(18),
        name="last",
    )(levels, c, tops, ix, tw, wi)


CHUNK = 4
CHUNKS = CX // CHUNK


def rebuild_kernel(in_ref, record_ref, mask_ref, table_ref, out_ref, made_ref, hold_ref, sems):
    def spread(group, carry):
        for k in range(8):
            f = group * 8 + k
            at = pl.ds(pl.multiple_of(f * PAD3, 8), 32)
            hold_ref[at, :] = in_ref[f].astype(F32) * (2.0 / NT)
        return carry

    lax.fori_loop(0, NF // 8, spread, 0)
    flags = lane_flags(mask_ref)

    def copy(i):
        part = pl.ds(i * CHUNK, CHUNK)
        return pltpu.make_async_copy(made_ref.at[part], out_ref.at[part], sems.at[i])

    for i in range(CHUNKS):
        for x in range(i * CHUNK, (i + 1) * CHUNK, 2):
            row = x // 2
            spec = jnp.concatenate(
                [hold_ref[pl.ds(p * 16 + row, NF, stride=PAD3), :] for p in range(2)], axis=0
            ).astype(BF16)
            recon = lax.dot_general(
                spec, table_ref[...], (((0,), (0,)), ((), ())), preferred_element_type=F32
            )
            kept = jnp.transpose(jnp.broadcast_to(flags[row : row + 1], (128, 128))) > 0
            rec = record_ref[x : x + 2].reshape(128, NT).astype(F32)
            for t in range(0, NT, 128):
                mixed = jnp.where(kept, rec[:, t : t + 128], recon[:, t : t + 128])
                made_ref[x : x + 2, :, t : t + 128] = mixed.astype(BF16).reshape(2, CY, 128)
        copy(i).start()
    for i in range(CHUNKS):
        copy(i).wait()


def rebuild(returned, record, sampled, table):
    return pl.pallas_call(
        rebuild_kernel,
        in_specs=[VMEM] * 4,
        out_specs=pl.BlockSpec(memory_space=pltpu.HBM),
        out_shape=jax.ShapeDtypeStruct((CX, CY, NT), BF16),
        scratch_shapes=[
            pltpu.VMEM((CX, CY, NT), BF16),
            pltpu.VMEM((NF * PAD3, 128), F32),
            pltpu.SemaphoreType.DMA((CHUNKS,)),
        ],
        compiler_params=limit(26),
        name="rebuild",
    )(returned, record, sampled, table)


def exchange(array):
    return lax.all_to_all(array, ALL, split_axis=0, concat_axis=0, tiled=True)


def tables():
    fx, ix = plane_tables()
    wf, wi = window_tables()
    narrow = [np.asarray(t, jnp.bfloat16) for t in (time_table(), fx, ix, wf, wi)]
    return (*narrow, np.asarray(twiddle_table(), np.float32))


def body(record, sampled, levels):
    time, fx, ix, wf, wi, tw = tables()
    sent = spectra_of(record, sampled)
    arrived = exchange(sent).reshape(NRX, TILES, ROWS, 128)
    flags = lax.ppermute(arrived[:, :, 32:40, :], ALL[2], [(0, 1), (1, 0)])
    c, top = first_half(arrived, fx, tw, wf)
    core = lax.axis_index(ALL[2]).reshape(1)
    top, flags, core = lax.optimization_barrier((top, flags, core))
    c, top = middle(levels, core, c, exchange(top), arrived, flags, fx, ix, tw, wf, wi)
    back = last_half(levels, c, exchange(top), ix, tw, wi)
    returned = exchange(back.reshape(NF, 32, 128))
    return rebuild(returned, record, sampled, time)


def solution(mesh):
    finer = Mesh(mesh.devices.reshape(2, 4, 2, 2, 4), ALL)
    rx, ry = ALL[:3], ALL[3:]
    return jax.shard_map(
        body,
        mesh=finer,
        in_specs=(P(rx, ry, None), P(rx, ry), P()),
        out_specs=P(rx, ry, None),
        check_vma=False,
    )
```

```python
import functools

import jax
import jax.numpy as jnp
import numpy as np
from jax import lax
from jax.experimental import pallas as pl
from jax.experimental.pallas import tpu as pltpu
from jax.sharding import Mesh
from jax.sharding import PartitionSpec as P

H = 16
NF = 128
FLO = 8
CX, CY, NT = 32, 64, 2048
LX = 512
HALF = LX // 2
QUARTER = LX // 4
TILES = 8
WIN = CY + 2 * H
NRX = LX // CX
ALL = ("rx_0", "rx_1", "rx_2", "ry_0", "ry_1")
F32 = jnp.float32
BF16 = jnp.bfloat16
PAD = 264
PAD3 = 40
SMEM = pl.BlockSpec(memory_space=pltpu.SMEM)
VMEM = pl.BlockSpec(memory_space=pltpu.VMEM)


def time_table():
    f = FLO + np.arange(NF)[:, None]
    ang = 2.0 * np.pi * (f * np.arange(NT)[None, :] % NT) / NT
    return np.concatenate([np.cos(ang), -np.sin(ang)], axis=0)


def plane_tables():
    a, m = np.arange(QUARTER)[None, :], np.arange(QUARTER)[:, None]
    blocks = []
    for odd in range(2):
        ang = 2.0 * np.pi * (a * (2 * m + odd) % HALF) / HALF
        c, s = np.cos(ang), np.sin(ang)
        blocks.append(np.block([[c, s], [-s, c]]))
    return np.concatenate(blocks), np.concatenate([b.T for b in blocks]) / LX


def twiddle_table():
    order = np.concatenate([np.arange(0, HALF, 2), np.arange(1, HALF, 2)])
    ang = 2.0 * np.pi * order[:, None] / LX
    ones = np.ones((HALF, CY))
    real = np.concatenate([ones, np.cos(ang) * ones], axis=1)
    imag = np.concatenate([0.0 * ones, -np.sin(ang) * ones], axis=1)
    return np.concatenate([real, imag], axis=0)


def taper():
    s = np.arange(WIN)
    rising = np.sin(0.5 * np.pi * (s + 0.5) / (2 * H))
    falling = np.cos(0.5 * np.pi * (s - CY + 0.5) / (2 * H))
    return np.where(s < 2 * H, rising, np.where(s >= CY, falling, 1.0))


def window_tables():
    k = np.arange(WIN)
    ang = 2.0 * np.pi * (k[:, None] * k[None, :] % WIN) / WIN
    w = taper()
    ya, yb = w[None, :] * np.cos(ang), w[None, :] * np.sin(ang)
    yc, yd = w[:, None] / WIN * np.cos(ang), w[:, None] / WIN * np.sin(ang)
    fwd = np.zeros((256, 256))
    inv = np.zeros((256, 256))
    for y in range(CY):
        spots = [(y, y + H)]
        if y < H:
            spots.append((128 + y, CY + H + y))
        if y >= CY - H:
            spots.append((128 + y, y - (CY - H)))
        for re, s in spots:
            im = re + CY
            fwd[re, :WIN] = ya[:, s]
            fwd[im, :WIN] = yb[:, s]
            fwd[im, 128 : 128 + WIN] = ya[:, s]
            fwd[re, 128 : 128 + WIN] = -yb[:, s]
            inv[:WIN, re] = yc[s, :]
            inv[128 : 128 + WIN, re] = -yd[s, :]
            inv[128 : 128 + WIN, im] = yc[s, :]
            inv[:WIN, im] = yd[s, :]
    return fwd, inv


MIB = 1024 * 1024
ROWS = 40


def limit(mib):
    return pltpu.CompilerParams(vmem_limit_bytes=int(mib * MIB))


def lane_flags(mask_ref):
    even = mask_ref[pl.ds(0, 16, stride=2), :]
    odd = mask_ref[pl.ds(1, 16, stride=2), :]
    return jnp.concatenate([even, odd], axis=1).astype(F32)


def make_time_table(table_ref):
    f = FLO + lax.broadcasted_iota(jnp.int32, (NF, 128), 0)
    n = lax.broadcasted_iota(jnp.int32, (NF, 128), 1)
    fine = (f * n % NT).astype(F32) * (2.0 * np.pi / NT)
    coarse = (f * n % (NT // 128)).astype(F32) * (2.0 * np.pi * 128 / NT)
    cos_fine, sin_fine = jnp.cos(fine), jnp.sin(fine)
    cos_coarse, sin_coarse = jnp.cos(coarse), jnp.sin(coarse)
    for u in range(NT // 128):
        c, s = cos_coarse[:, u : u + 1], sin_coarse[:, u : u + 1]
        at = u * 128
        table_ref[:NF, at : at + 128] = (c * cos_fine - s * sin_fine).astype(BF16)
        table_ref[NF:, at : at + 128] = (-(s * cos_fine + c * sin_fine)).astype(BF16)


def spectra_kernel(record_ref, hold_ref, in_ref, table_ref, sems):
    chunk, ahead = 8, 3
    chunks = CX // chunk

    def copy(i):
        part = pl.ds(i * chunk, chunk)
        return pltpu.make_async_copy(record_ref.at[part], in_ref.at[part], sems.at[i])

    for i in range(ahead):
        copy(i).start()
    make_time_table(table_ref)

    def transform(i, carry):
        copy(i).wait()

        @pl.when(i + ahead < chunks)
        def _():
            copy(i + ahead).start()

        traces = in_ref[pl.ds(i * chunk, chunk)].reshape(-1, NT)
        res = lax.dot_general(
            table_ref[...], traces, (((1,), (1,)), ((), ())), preferred_element_type=F32
        )
        for b in range(chunk // 2):
            row = i * (chunk // 2) + b
            at = pl.ds(pl.multiple_of(row * PAD, 8), 2 * NF)
            hold_ref[at, :] = res[:, b * 128 : (b + 1) * 128]
        return carry

    lax.fori_loop(0, chunks, transform, 0)


def place_kernel(hold_ref, mask_ref, out_ref):
    flags = lane_flags(mask_ref)
    kept = flags > 0
    halves = [flags[c * 8 : (c + 1) * 8].astype(BF16) for c in range(2)]

    def place(group, carry):
        for k in range(16):
            f = group * 16 + k
            for p in range(2):
                part = hold_ref[pl.ds(p * NF + f, 16, stride=PAD), :]
                out_ref[f, p * 16 : (p + 1) * 16, :] = jnp.where(kept, part, 0.0).astype(BF16)
            out_ref[f, 32:40, :] = halves[k // 8]
        return carry

    lax.fori_loop(0, NF // 16, place, 0)


def spectra_of(record, sampled):
    hold = pl.pallas_call(
        spectra_kernel,
        in_specs=[pl.BlockSpec(memory_space=pltpu.HBM)],
        out_specs=VMEM,
        out_shape=jax.ShapeDtypeStruct((16 * PAD, 128), F32),
        scratch_shapes=[
            pltpu.VMEM((CX, CY, NT), BF16),
            pltpu.VMEM((2 * NF, NT), BF16),
            pltpu.SemaphoreType.DMA((CX // 8,)),
        ],
        compiler_params=limit(51),
        name="spectra",
    )(record)
    return pl.pallas_call(
        place_kernel,
        in_specs=[VMEM, VMEM],
        out_specs=VMEM,
        out_shape=jax.ShapeDtypeStruct((NF, ROWS, 128), BF16),
        compiler_params=limit(40),
        name="place",
    )(hold, sampled)


GROUP = 4


def early_lanes(rows):
    return lax.broadcasted_iota(jnp.int32, (rows, 128), 1) % CY < CY // 2


def low_lanes():
    return lax.broadcasted_iota(jnp.int32, (QUARTER, 128), 1) < CY


def side_by_side(blocks):
    return jnp.concatenate(blocks, axis=1)


def columns_of(in_ref, ry, p):
    return in_ref[:, ry, p * 16 : (p + 1) * 16, :].reshape(HALF, 128)


def forward_columns(parts, fx_ref, tw_ref, v_ref, start):
    low = low_lanes()
    for odd in range(2):
        upper, lower = [x[:QUARTER] for x in parts], [x[QUARTER:] for x in parts]
        data = jnp.concatenate([u - w if odd else u + w for u, w in zip(upper, lower)], axis=0)
        table = fx_ref[odd * HALF : (odd + 1) * HALF]
        res = jnp.dot(table, data, preferred_element_type=F32)
        rows = odd * QUARTER
        tr = tw_ref[rows : rows + QUARTER]
        ti = tw_ref[HALF + rows : HALF + rows + QUARTER]
        for k in range(GROUP):
            at = k * 128
            ar, ai = res[:QUARTER, at : at + 128], res[QUARTER:, at : at + 128]
            br = ar * tr - ai * ti
            bi = ar * ti + ai * tr
            first = jnp.where(low, br, pltpu.roll(bi, CY, 1))
            second = jnp.where(low, pltpu.roll(br, CY, 1), bi)
            v_ref[start + k, rows : rows + QUARTER] = (first + second).astype(BF16)
            v_ref[start + k, HALF + rows : HALF + rows + QUARTER] = (first - second).astype(BF16)


def forward_tiles(v_ref, wf_ref, c_ref):
    early = early_lanes(LX)
    best = jnp.zeros((8, 128), F32)
    for j in range(TILES):
        left, right = (j + TILES - 1) % TILES, (j + 1) % TILES
        near = jnp.where(early, v_ref[right], v_ref[left])
        c = jnp.dot(side_by_side([v_ref[j], near]), wf_ref[...], preferred_element_type=F32)
        c_ref[j] = c
        squares = c[:, :128] * c[:, :128] + c[:, 128:] * c[:, 128:]
        best = jnp.maximum(best, jnp.max(squares.reshape(-1, 8, 128), axis=0))
    return best


def put_largest(best, top_ref):
    top = jnp.sqrt(jnp.max(best, keepdims=True))
    top_ref[...] = jnp.broadcast_to(top, top_ref.shape)


def shrink_tiles(c_ref, tops_ref, level, wi_ref, o_ref):
    tau = level.astype(F32) * 0.001 * (
        jnp.max(tops_ref[...], axis=0, keepdims=True) + 1e-06
    )
    for j in range(TILES):
        real, imag = c_ref[j, :, :128], c_ref[j, :, 128:]
        g = jnp.maximum(1.0 - tau * lax.rsqrt(real * real + imag * imag), 0.0)
        e = side_by_side([real * g, imag * g]).astype(BF16)
        o_ref[j] = jnp.dot(e, wi_ref[...], preferred_element_type=F32)


def inverse_columns(o_ref, ix_ref, tw_ref, start):
    low, early = low_lanes(), early_lanes(QUARTER)
    made = []
    for odd in range(2):
        rows = odd * QUARTER
        tr = tw_ref[rows : rows + QUARTER]
        ti = tw_ref[HALF + rows : HALF + rows + QUARTER]
        reals, imags = [], []
        for j in range(start, start + GROUP):
            left, right = (j + TILES - 1) % TILES, (j + 1) % TILES
            halves = []
            for at in (rows, HALF + rows):
                part = pl.ds(at, QUARTER)
                near = jnp.where(early, o_ref[left, part, 128:], o_ref[right, part, 128:])
                halves.append(o_ref[j, part, :128] + near)
            total, apart = halves[0] + halves[1], halves[0] - halves[1]
            real = jnp.where(low, total, pltpu.roll(apart, CY, 1))
            imag = jnp.where(low, pltpu.roll(total, CY, 1), apart)
            reals.append((real * tr + imag * ti).astype(BF16))
            imags.append((imag * tr - real * ti).astype(BF16))
        g = jnp.concatenate([side_by_side(reals), side_by_side(imags)], axis=0)
        table = ix_ref[odd * HALF : (odd + 1) * HALF]
        made.append(jnp.dot(table, g, preferred_element_type=F32))
    even, odd = made
    return [
        jnp.concatenate([even[at : at + QUARTER] + odd[at : at + QUARTER],
                         even[at : at + QUARTER] - odd[at : at + QUARTER]], axis=0).astype(BF16)
        for at in (0, QUARTER)
    ]


def first_kernel(in_ref, fx_ref, tw_ref, wf_ref, c_ref, top_ref, v_ref):
    for start in range(0, TILES, GROUP):
        parts = [
            side_by_side([columns_of(in_ref, start + k, p) for k in range(GROUP)])
            for p in range(2)
        ]
        forward_columns(parts, fx_ref, tw_ref, v_ref, start)
    put_largest(forward_tiles(v_ref, wf_ref, c_ref), top_ref)


def middle_kernel(
    level_ref, core_ref, c_ref, tops_ref, in_ref, flag_ref, fx_ref, ix_ref, tw_ref, wf_ref, wi_ref,
    c2_ref, top_ref, o_ref, v_ref,
):
    shrink_tiles(c_ref, tops_ref, level_ref[0], wi_ref, o_ref)
    on_first = core_ref[0] == 0
    for start in range(0, TILES, GROUP):
        fresh = inverse_columns(o_ref, ix_ref, tw_ref, start)
        kept = []
        for k in range(GROUP):
            mine = in_ref[:, start + k, 32:40, :].astype(F32)
            other = flag_ref[:, start + k].astype(F32)
            upper, lower = jnp.where(on_first, mine, other), jnp.where(on_first, other, mine)
            kept.append(jnp.concatenate([upper, lower], axis=1).reshape(HALF, 128))
        kept = side_by_side(kept) > 0
        parts = []
        for p in range(2):
            sent = side_by_side([columns_of(in_ref, start + k, p) for k in range(GROUP)])
            parts.append(jnp.where(kept, sent, fresh[p]))
        forward_columns(parts, fx_ref, tw_ref, v_ref, start)
    put_largest(forward_tiles(v_ref, wf_ref, c2_ref), top_ref)


def last_kernel(level_ref, c_ref, tops_ref, ix_ref, tw_ref, wi_ref, out_ref, o_ref):
    shrink_tiles(c_ref, tops_ref, level_ref[1], wi_ref, o_ref)
    for start in range(0, TILES, GROUP):
        fresh = inverse_columns(o_ref, ix_ref, tw_ref, start)
        for k in range(GROUP):
            for p in range(2):
                part = fresh[p][:, k * 128 : (k + 1) * 128]
                out_ref[:, start + k, p * 16 : (p + 1) * 16, :] = part.reshape(NRX, 16, 128)


COEFFS = jax.ShapeDtypeStruct((TILES, LX, 256), F32)
TOPS = jax.ShapeDtypeStruct((NF, 128), F32)
V_SCRATCH = pltpu.VMEM((TILES, LX, 128), BF16)
O_SCRATCH = pltpu.VMEM((TILES, LX, 256), F32)


def first_half(arrived, fx, tw, wf):
    return pl.pallas_call(
        first_kernel,
        in_specs=[VMEM] * 4,
        out_specs=[VMEM] * 2,
        out_shape=[COEFFS, TOPS],
        scratch_shapes=[V_SCRATCH],
        compiler_params=limit(18),
        name="first",
    )(arrived, fx, tw, wf)


def middle(levels, core, c, tops, arrived, flags, fx, ix, tw, wf, wi):
    return pl.pallas_call(
        middle_kernel,
        in_specs=[SMEM] * 2 + [VMEM] * 9,
        out_specs=[VMEM] * 2,
        out_shape=[COEFFS, TOPS],
        scratch_shapes=[O_SCRATCH, V_SCRATCH],
        compiler_params=limit(26),
        name="middle",
    )(levels, core, c, tops, arrived, flags, fx, ix, tw, wf, wi)


def last_half(levels, c, tops, ix, tw, wi):
    return pl.pallas_call(
        last_kernel,
        in_specs=[SMEM] + [VMEM] * 5,
        out_specs=VMEM,
        out_shape=jax.ShapeDtypeStruct((NRX, TILES, 32, 128), BF16),
        scratch_shapes=[O_SCRATCH],
        compiler_params=limit(18),
        name="last",
    )(levels, c, tops, ix, tw, wi)


CHUNK = 4
CHUNKS = CX // CHUNK


def rebuild_kernel(in_ref, record_ref, mask_ref, table_ref, out_ref, made_ref, hold_ref, sems):
    def spread(group, carry):
        for k in range(8):
            f = group * 8 + k
            at = pl.ds(pl.multiple_of(f * PAD3, 8), 32)
            hold_ref[at, :] = in_ref[f].astype(F32) * (2.0 / NT)
        return carry

    lax.fori_loop(0, NF // 8, spread, 0)
    flags = lane_flags(mask_ref)

    def copy(i):
        part = pl.ds(i * CHUNK, CHUNK)
        return pltpu.make_async_copy(made_ref.at[part], out_ref.at[part], sems.at[i])

    for i in range(CHUNKS):
        for x in range(i * CHUNK, (i + 1) * CHUNK, 2):
            row = x // 2
            spec = jnp.concatenate(
                [hold_ref[pl.ds(p * 16 + row, NF, stride=PAD3), :] for p in range(2)], axis=0
            ).astype(BF16)
            recon = lax.dot_general(
                spec, table_ref[...], (((0,), (0,)), ((), ())), preferred_element_type=F32
            )
            kept = jnp.transpose(jnp.broadcast_to(flags[row : row + 1], (128, 128))) > 0
            rec = record_ref[x : x + 2].reshape(128, NT).astype(F32)
            for t in range(0, NT, 128):
                mixed = jnp.where(kept, rec[:, t : t + 128], recon[:, t : t + 128])
                made_ref[x : x + 2, :, t : t + 128] = mixed.astype(BF16).reshape(2, CY, 128)
        copy(i).start()
    for i in range(CHUNKS):
        copy(i).wait()


def rebuild(returned, record, sampled, table):
    return pl.pallas_call(
        rebuild_kernel,
        in_specs=[VMEM] * 4,
        out_specs=pl.BlockSpec(memory_space=pltpu.HBM),
        out_shape=jax.ShapeDtypeStruct((CX, CY, NT), BF16),
        scratch_shapes=[
            pltpu.VMEM((CX, CY, NT), BF16),
            pltpu.VMEM((NF * PAD3, 128), F32),
            pltpu.SemaphoreType.DMA((CHUNKS,)),
        ],
        compiler_params=limit(26),
        name="rebuild",
    )(returned, record, sampled, table)


def exchange(array):
    return lax.all_to_all(array, ALL, split_axis=0, concat_axis=0, tiled=True)


def all_tops(top):
    return exchange(top.reshape(NF, 1, 128)).reshape(NF, 128)


def tables():
    fx, ix = plane_tables()
    wf, wi = window_tables()
    narrow = [np.asarray(t, jnp.bfloat16) for t in (time_table(), fx, ix, wf, wi)]
    return (*narrow, np.asarray(twiddle_table(), np.float32))


def body(record, sampled, levels):
    time, fx, ix, wf, wi, tw = tables()
    sent = spectra_of(record, sampled)
    arrived = exchange(sent).reshape(NRX, TILES, ROWS, 128)
    flags = lax.ppermute(arrived[:, :, 32:40, :], ALL[2], [(0, 1), (1, 0)])
    c, top = first_half(arrived, fx, tw, wf)
    core = lax.axis_index(ALL[2]).reshape(1)
    top, flags, core = lax.optimization_barrier((top, flags, core))
    c, top = middle(levels, core, c, all_tops(top), arrived, flags, fx, ix, tw, wf, wi)
    back = last_half(levels, c, all_tops(top), ix, tw, wi)
    returned = exchange(back.reshape(NF, 32, 128))
    return rebuild(returned, record, sampled, time)


def solution(mesh):
    finer = Mesh(mesh.devices.reshape(2, 4, 2, 2, 4), ALL)
    rx, ry = ALL[:3], ALL[3:]
    return jax.shard_map(
        body,
        mesh=finer,
        in_specs=(P(rx, ry, None), P(rx, ry), P()),
        out_specs=P(rx, ry, None),
        check_vma=False,
    )
```

```python
import functools

import jax
import jax.numpy as jnp
import numpy as np
from jax import lax
from jax.experimental import pallas as pl
from jax.experimental.pallas import tpu as pltpu
from jax.sharding import Mesh
from jax.sharding import PartitionSpec as P

H = 16
NF = 128
FLO = 8
CX, CY, NT = 32, 64, 2048
LX = 512
HALF = LX // 2
QUARTER = LX // 4
TILES = 8
WIN = CY + 2 * H
NRX = LX // CX
ALL = ("rx_0", "rx_1", "rx_2", "ry_0", "ry_1")
F32 = jnp.float32
BF16 = jnp.bfloat16
PAD = 264
PAD3 = 40
SMEM = pl.BlockSpec(memory_space=pltpu.SMEM)
VMEM = pl.BlockSpec(memory_space=pltpu.VMEM)


def time_table():
    f = FLO + np.arange(NF)[:, None]
    ang = 2.0 * np.pi * (f * np.arange(NT)[None, :] % NT) / NT
    return np.concatenate([np.cos(ang), -np.sin(ang)], axis=0)


def plane_tables():
    a, m = np.arange(QUARTER)[None, :], np.arange(QUARTER)[:, None]
    blocks = []
    for odd in range(2):
        ang = 2.0 * np.pi * (a * (2 * m + odd) % HALF) / HALF
        c, s = np.cos(ang), np.sin(ang)
        blocks.append(np.block([[c, s], [-s, c]]))
    return np.concatenate(blocks), np.concatenate([b.T for b in blocks]) / LX


def twiddle_table():
    order = np.concatenate([np.arange(0, HALF, 2), np.arange(1, HALF, 2)])
    ang = 2.0 * np.pi * order[:, None] / LX
    ones = np.ones((HALF, CY))
    real = np.concatenate([ones, np.cos(ang) * ones], axis=1)
    imag = np.concatenate([0.0 * ones, -np.sin(ang) * ones], axis=1)
    return np.concatenate([real, imag], axis=0)


def taper():
    s = np.arange(WIN)
    rising = np.sin(0.5 * np.pi * (s + 0.5) / (2 * H))
    falling = np.cos(0.5 * np.pi * (s - CY + 0.5) / (2 * H))
    return np.where(s < 2 * H, rising, np.where(s >= CY, falling, 1.0))


def window_tables():
    k = np.arange(WIN)
    ang = 2.0 * np.pi * (k[:, None] * k[None, :] % WIN) / WIN
    w = taper()
    ya, yb = w[None, :] * np.cos(ang), w[None, :] * np.sin(ang)
    yc, yd = w[:, None] / WIN * np.cos(ang), w[:, None] / WIN * np.sin(ang)
    fwd = np.zeros((256, 256))
    inv = np.zeros((256, 256))
    for y in range(CY):
        spots = [(y, y + H)]
        if y < H:
            spots.append((128 + y, CY + H + y))
        if y >= CY - H:
            spots.append((128 + y, y - (CY - H)))
        for re, s in spots:
            im = re + CY
            fwd[re, :WIN] = ya[:, s]
            fwd[im, :WIN] = yb[:, s]
            fwd[im, 128 : 128 + WIN] = ya[:, s]
            fwd[re, 128 : 128 + WIN] = -yb[:, s]
            inv[:WIN, re] = yc[s, :]
            inv[128 : 128 + WIN, re] = -yd[s, :]
            inv[128 : 128 + WIN, im] = yc[s, :]
            inv[:WIN, im] = yd[s, :]
    return fwd, inv


MIB = 1024 * 1024
ROWS = 40


def limit(mib):
    return pltpu.CompilerParams(vmem_limit_bytes=int(mib * MIB))


def lane_flags(mask_ref):
    even = mask_ref[pl.ds(0, 16, stride=2), :]
    odd = mask_ref[pl.ds(1, 16, stride=2), :]
    return jnp.concatenate([even, odd], axis=1).astype(F32)


def make_time_table(table_ref):
    f = FLO + lax.broadcasted_iota(jnp.int32, (NF, 128), 0)
    n = lax.broadcasted_iota(jnp.int32, (NF, 128), 1)
    fine = (f * n % NT).astype(F32) * (2.0 * np.pi / NT)
    coarse = (f * n % (NT // 128)).astype(F32) * (2.0 * np.pi * 128 / NT)
    cos_fine, sin_fine = jnp.cos(fine), jnp.sin(fine)
    cos_coarse, sin_coarse = jnp.cos(coarse), jnp.sin(coarse)
    for u in range(NT // 128):
        c, s = cos_coarse[:, u : u + 1], sin_coarse[:, u : u + 1]
        at = u * 128
        table_ref[:NF, at : at + 128] = (c * cos_fine - s * sin_fine).astype(BF16)
        table_ref[NF:, at : at + 128] = (-(s * cos_fine + c * sin_fine)).astype(BF16)


def spectra_kernel(record_ref, hold_ref, in_ref, table_ref, sems):
    chunk, ahead = 8, 4
    chunks = CX // chunk

    def copy(i):
        part = pl.ds(i * chunk, chunk)
        return pltpu.make_async_copy(record_ref.at[part], in_ref.at[part], sems.at[i])

    for i in range(ahead):
        copy(i).start()
    make_time_table(table_ref)

    def transform(i, carry):
        copy(i).wait()

        traces = in_ref[pl.ds(i * chunk, chunk)].reshape(-1, NT)
        res = lax.dot_general(
            table_ref[...], traces, (((1,), (1,)), ((), ())), preferred_element_type=F32
        )
        for b in range(chunk // 2):
            row = i * (chunk // 2) + b
            at = pl.ds(pl.multiple_of(row * PAD, 8), 2 * NF)
            hold_ref[at, :] = res[:, b * 128 : (b + 1) * 128]
        return carry

    lax.fori_loop(0, chunks, transform, 0)


def place_kernel(hold_ref, mask_ref, out_ref):
    flags = lane_flags(mask_ref)
    kept = flags > 0
    halves = [flags[c * 8 : (c + 1) * 8].astype(BF16) for c in range(2)]

    def place(group, carry):
        for k in range(16):
            f = group * 16 + k
            for p in range(2):
                part = hold_ref[pl.ds(p * NF + f, 16, stride=PAD), :]
                out_ref[f, p * 16 : (p + 1) * 16, :] = jnp.where(kept, part, 0.0).astype(BF16)
            out_ref[f, 32:40, :] = halves[k // 8]
        return carry

    lax.fori_loop(0, NF // 16, place, 0)


def spectra_of(record, sampled):
    hold = pl.pallas_call(
        spectra_kernel,
        in_specs=[pl.BlockSpec(memory_space=pltpu.HBM)],
        out_specs=VMEM,
        out_shape=jax.ShapeDtypeStruct((16 * PAD, 128), F32),
        scratch_shapes=[
            pltpu.VMEM((CX, CY, NT), BF16),
            pltpu.VMEM((2 * NF, NT), BF16),
            pltpu.SemaphoreType.DMA((CX // 8,)),
        ],
        compiler_params=limit(51),
        name="spectra",
    )(record)
    return pl.pallas_call(
        place_kernel,
        in_specs=[VMEM, VMEM],
        out_specs=VMEM,
        out_shape=jax.ShapeDtypeStruct((NF, ROWS, 128), BF16),
        compiler_params=limit(40),
        name="place",
    )(hold, sampled)


GROUP = 4


def early_lanes(rows):
    return lax.broadcasted_iota(jnp.int32, (rows, 128), 1) % CY < CY // 2


def low_lanes():
    return lax.broadcasted_iota(jnp.int32, (QUARTER, 128), 1) < CY


def side_by_side(blocks):
    return jnp.concatenate(blocks, axis=1)


def columns_of(in_ref, ry, p):
    return in_ref[:, ry, p * 16 : (p + 1) * 16, :].reshape(HALF, 128)


def forward_columns(parts, fx_ref, tw_ref, v_ref, start):
    low = low_lanes()
    for odd in range(2):
        upper, lower = [x[:QUARTER] for x in parts], [x[QUARTER:] for x in parts]
        data = jnp.concatenate([u - w if odd else u + w for u, w in zip(upper, lower)], axis=0)
        table = fx_ref[odd * HALF : (odd + 1) * HALF]
        res = jnp.dot(table, data, preferred_element_type=F32)
        rows = odd * QUARTER
        tr = tw_ref[rows : rows + QUARTER]
        ti = tw_ref[HALF + rows : HALF + rows + QUARTER]
        for k in range(GROUP):
            at = k * 128
            ar, ai = res[:QUARTER, at : at + 128], res[QUARTER:, at : at + 128]
            br = ar * tr - ai * ti
            bi = ar * ti + ai * tr
            first = jnp.where(low, br, pltpu.roll(bi, CY, 1))
            second = jnp.where(low, pltpu.roll(br, CY, 1), bi)
            v_ref[start + k, rows : rows + QUARTER] = (first + second).astype(BF16)
            v_ref[start + k, HALF + rows : HALF + rows + QUARTER] = (first - second).astype(BF16)


def forward_tiles(v_ref, wf_ref, c_ref):
    early = early_lanes(LX)
    best = jnp.zeros((8, 128), F32)
    for j in range(TILES):
        left, right = (j + TILES - 1) % TILES, (j + 1) % TILES
        near = jnp.where(early, v_ref[right], v_ref[left])
        c = jnp.dot(side_by_side([v_ref[j], near]), wf_ref[...], preferred_element_type=F32)
        c_ref[j] = c
        squares = c[:, :128] * c[:, :128] + c[:, 128:] * c[:, 128:]
        best = jnp.maximum(best, jnp.max(squares.reshape(-1, 8, 128), axis=0))
    return best


def put_largest(best, top_ref):
    top = jnp.sqrt(jnp.max(best, keepdims=True))
    top_ref[...] = jnp.broadcast_to(top, top_ref.shape)


def shrink_tiles(c_ref, tops_ref, level, wi_ref, o_ref):
    tau = level.astype(F32) * 0.001 * (
        jnp.max(tops_ref[...], axis=0, keepdims=True) + 1e-06
    )
    for j in range(TILES):
        real, imag = c_ref[j, :, :128], c_ref[j, :, 128:]
        g = jnp.maximum(1.0 - tau * lax.rsqrt(real * real + imag * imag), 0.0)
        e = side_by_side([real * g, imag * g]).astype(BF16)
        o_ref[j] = jnp.dot(e, wi_ref[...], preferred_element_type=F32)


def inverse_columns(o_ref, ix_ref, tw_ref, start):
    low, early = low_lanes(), early_lanes(QUARTER)
    made = []
    for odd in range(2):
        rows = odd * QUARTER
        tr = tw_ref[rows : rows + QUARTER]
        ti = tw_ref[HALF + rows : HALF + rows + QUARTER]
        reals, imags = [], []
        for j in range(start, start + GROUP):
            left, right = (j + TILES - 1) % TILES, (j + 1) % TILES
            halves = []
            for at in (rows, HALF + rows):
                part = pl.ds(at, QUARTER)
                near = jnp.where(early, o_ref[left, part, 128:], o_ref[right, part, 128:])
                halves.append(o_ref[j, part, :128] + near)
            total, apart = halves[0] + halves[1], halves[0] - halves[1]
            real = jnp.where(low, total, pltpu.roll(apart, CY, 1))
            imag = jnp.where(low, pltpu.roll(total, CY, 1), apart)
            reals.append((real * tr + imag * ti).astype(BF16))
            imags.append((imag * tr - real * ti).astype(BF16))
        g = jnp.concatenate([side_by_side(reals), side_by_side(imags)], axis=0)
        table = ix_ref[odd * HALF : (odd + 1) * HALF]
        made.append(jnp.dot(table, g, preferred_element_type=F32))
    even, odd = made
    return [
        jnp.concatenate([even[at : at + QUARTER] + odd[at : at + QUARTER],
                         even[at : at + QUARTER] - odd[at : at + QUARTER]], axis=0).astype(BF16)
        for at in (0, QUARTER)
    ]


def first_kernel(in_ref, fx_ref, tw_ref, wf_ref, c_ref, top_ref, v_ref):
    for start in range(0, TILES, GROUP):
        parts = [
            side_by_side([columns_of(in_ref, start + k, p) for k in range(GROUP)])
            for p in range(2)
        ]
        forward_columns(parts, fx_ref, tw_ref, v_ref, start)
    put_largest(forward_tiles(v_ref, wf_ref, c_ref), top_ref)


def middle_kernel(
    level_ref, core_ref, c_ref, tops_ref, in_ref, flag_ref, fx_ref, ix_ref, tw_ref, wf_ref, wi_ref,
    c2_ref, top_ref, o_ref, v_ref,
):
    shrink_tiles(c_ref, tops_ref, level_ref[0], wi_ref, o_ref)
    on_first = core_ref[0] == 0
    for start in range(0, TILES, GROUP):
        fresh = inverse_columns(o_ref, ix_ref, tw_ref, start)
        kept = []
        for k in range(GROUP):
            mine = in_ref[:, start + k, 32:40, :]
            other = flag_ref[:, start + k]
            upper, lower = jnp.where(on_first, mine, other), jnp.where(on_first, other, mine)
            kept.append(jnp.concatenate([upper, lower], axis=1).reshape(HALF, 128))
        kept = side_by_side(kept) > 0
        parts = []
        for p in range(2):
            sent = side_by_side([columns_of(in_ref, start + k, p) for k in range(GROUP)])
            parts.append(jnp.where(kept, sent, fresh[p]))
        forward_columns(parts, fx_ref, tw_ref, v_ref, start)
    put_largest(forward_tiles(v_ref, wf_ref, c2_ref), top_ref)


def last_kernel(level_ref, c_ref, tops_ref, ix_ref, tw_ref, wi_ref, out_ref, o_ref):
    shrink_tiles(c_ref, tops_ref, level_ref[1], wi_ref, o_ref)
    for start in range(0, TILES, GROUP):
        fresh = inverse_columns(o_ref, ix_ref, tw_ref, start)
        for k in range(GROUP):
            for p in range(2):
                part = fresh[p][:, k * 128 : (k + 1) * 128]
                out_ref[:, start + k, p * 16 : (p + 1) * 16, :] = part.reshape(NRX, 16, 128)


COEFFS = jax.ShapeDtypeStruct((TILES, LX, 256), F32)
TOPS = jax.ShapeDtypeStruct((NF, 128), F32)
V_SCRATCH = pltpu.VMEM((TILES, LX, 128), BF16)
O_SCRATCH = pltpu.VMEM((TILES, LX, 256), F32)


def first_half(arrived, fx, tw, wf):
    return pl.pallas_call(
        first_kernel,
        in_specs=[VMEM] * 4,
        out_specs=[VMEM] * 2,
        out_shape=[COEFFS, TOPS],
        scratch_shapes=[V_SCRATCH],
        compiler_params=limit(18),
        name="first",
    )(arrived, fx, tw, wf)


def middle(levels, core, c, tops, arrived, flags, fx, ix, tw, wf, wi):
    return pl.pallas_call(
        middle_kernel,
        in_specs=[SMEM] * 2 + [VMEM] * 9,
        out_specs=[VMEM] * 2,
        out_shape=[COEFFS, TOPS],
        scratch_shapes=[O_SCRATCH, V_SCRATCH],
        compiler_params=limit(26),
        name="middle",
    )(levels, core, c, tops, arrived, flags, fx, ix, tw, wf, wi)


def last_half(levels, c, tops, ix, tw, wi):
    return pl.pallas_call(
        last_kernel,
        in_specs=[SMEM] + [VMEM] * 5,
        out_specs=VMEM,
        out_shape=jax.ShapeDtypeStruct((NRX, TILES, 32, 128), BF16),
        scratch_shapes=[O_SCRATCH],
        compiler_params=limit(18),
        name="last",
    )(levels, c, tops, ix, tw, wi)


CHUNK = 4
CHUNKS = CX // CHUNK


def rebuild_kernel(in_ref, record_ref, mask_ref, table_ref, out_ref, made_ref, hold_ref, sems):
    def spread(group, carry):
        for k in range(8):
            f = group * 8 + k
            at = pl.ds(pl.multiple_of(f * PAD3, 8), 32)
            hold_ref[at, :] = in_ref[f].astype(F32) * (2.0 / NT)
        return carry

    lax.fori_loop(0, NF // 8, spread, 0, unroll=4)
    flags = lane_flags(mask_ref)

    def copy(i):
        part = pl.ds(i * CHUNK, CHUNK)
        return pltpu.make_async_copy(made_ref.at[part], out_ref.at[part], sems.at[i])

    for i in range(CHUNKS):
        for x in range(i * CHUNK, (i + 1) * CHUNK, 2):
            row = x // 2
            spec = jnp.concatenate(
                [hold_ref[pl.ds(p * 16 + row, NF, stride=PAD3), :] for p in range(2)], axis=0
            ).astype(BF16)
            recon = lax.dot_general(
                spec, table_ref[...], (((0,), (0,)), ((), ())), preferred_element_type=F32
            )
            kept = jnp.transpose(jnp.broadcast_to(flags[row : row + 1], (128, 128))) > 0
            rec = record_ref[x : x + 2].reshape(128, NT).astype(F32)
            for t in range(0, NT, 128):
                mixed = jnp.where(kept, rec[:, t : t + 128], recon[:, t : t + 128])
                made_ref[x : x + 2, :, t : t + 128] = mixed.astype(BF16).reshape(2, CY, 128)
        copy(i).start()
    for i in range(CHUNKS):
        copy(i).wait()


def rebuild(returned, record, sampled, table):
    return pl.pallas_call(
        rebuild_kernel,
        in_specs=[VMEM] * 4,
        out_specs=pl.BlockSpec(memory_space=pltpu.HBM),
        out_shape=jax.ShapeDtypeStruct((CX, CY, NT), BF16),
        scratch_shapes=[
            pltpu.VMEM((CX, CY, NT), BF16),
            pltpu.VMEM((NF * PAD3, 128), F32),
            pltpu.SemaphoreType.DMA((CHUNKS,)),
        ],
        compiler_params=limit(26),
        name="rebuild",
    )(returned, record, sampled, table)


def exchange(array):
    return lax.all_to_all(array, ALL, split_axis=0, concat_axis=0, tiled=True)


def all_tops(top):
    return exchange(top.reshape(NF, 1, 128)).reshape(NF, 128)


def tables():
    fx, ix = plane_tables()
    wf, wi = window_tables()
    narrow = [np.asarray(t, jnp.bfloat16) for t in (time_table(), fx, ix, wf, wi)]
    return (*narrow, np.asarray(twiddle_table(), np.float32))


def body(record, sampled, levels):
    time, fx, ix, wf, wi, tw = tables()
    sent = spectra_of(record, sampled)
    arrived = exchange(sent).reshape(NRX, TILES, ROWS, 128)
    flags = lax.ppermute(arrived[:, :, 32:40, :], ALL[2], [(0, 1), (1, 0)])
    c, top = first_half(arrived, fx, tw, wf)
    core = lax.axis_index(ALL[2]).reshape(1)
    top, flags, core = lax.optimization_barrier((top, flags, core))
    c, top = middle(levels, core, c, all_tops(top), arrived, flags, fx, ix, tw, wf, wi)
    back = last_half(levels, c, all_tops(top), ix, tw, wi)
    returned = exchange(back.reshape(NF, 32, 128))
    return rebuild(returned, record, sampled, time)


def solution(mesh):
    finer = Mesh(mesh.devices.reshape(2, 4, 2, 2, 4), ALL)
    rx, ry = ALL[:3], ALL[3:]
    return jax.shard_map(
        body,
        mesh=finer,
        in_specs=(P(rx, ry, None), P(rx, ry), P()),
        out_specs=P(rx, ry, None),
        check_vma=False,
    )
```

```python
import functools

import jax
import jax.numpy as jnp
import numpy as np
from jax import lax
from jax.experimental import pallas as pl
from jax.experimental.pallas import tpu as pltpu
from jax.sharding import Mesh
from jax.sharding import PartitionSpec as P

H = 16
NF = 128
FLO = 8
CX, CY, NT = 32, 64, 2048
LX = 512
HALF = LX // 2
QUARTER = LX // 4
TILES = 8
WIN = CY + 2 * H
NRX = LX // CX
ALL = ("rx_0", "rx_1", "rx_2", "ry_0", "ry_1")
F32 = jnp.float32
BF16 = jnp.bfloat16
PAD = 264
PAD3 = 40
SMEM = pl.BlockSpec(memory_space=pltpu.SMEM)
VMEM = pl.BlockSpec(memory_space=pltpu.VMEM)


def time_table():
    f = FLO + np.arange(NF)[:, None]
    ang = 2.0 * np.pi * (f * np.arange(NT)[None, :] % NT) / NT
    return np.concatenate([np.cos(ang), -np.sin(ang)], axis=0)


def plane_tables():
    a, m = np.arange(QUARTER)[None, :], np.arange(QUARTER)[:, None]
    blocks = []
    for odd in range(2):
        ang = 2.0 * np.pi * (a * (2 * m + odd) % HALF) / HALF
        c, s = np.cos(ang), np.sin(ang)
        blocks.append(np.block([[c, s], [-s, c]]))
    return np.concatenate(blocks), np.concatenate([b.T for b in blocks]) / LX


def twiddle_table():
    order = np.concatenate([np.arange(0, HALF, 2), np.arange(1, HALF, 2)])
    ang = 2.0 * np.pi * order[:, None] / LX
    ones = np.ones((HALF, CY))
    real = np.concatenate([ones, np.cos(ang) * ones], axis=1)
    imag = np.concatenate([0.0 * ones, -np.sin(ang) * ones], axis=1)
    return np.concatenate([real, imag], axis=0)


def taper():
    s = np.arange(WIN)
    rising = np.sin(0.5 * np.pi * (s + 0.5) / (2 * H))
    falling = np.cos(0.5 * np.pi * (s - CY + 0.5) / (2 * H))
    return np.where(s < 2 * H, rising, np.where(s >= CY, falling, 1.0))


def window_tables():
    k = np.arange(WIN)
    ang = 2.0 * np.pi * (k[:, None] * k[None, :] % WIN) / WIN
    w = taper()
    ya, yb = w[None, :] * np.cos(ang), w[None, :] * np.sin(ang)
    yc, yd = w[:, None] / WIN * np.cos(ang), w[:, None] / WIN * np.sin(ang)
    fwd = np.zeros((256, 256))
    inv = np.zeros((256, 256))
    for y in range(CY):
        spots = [(y, y + H)]
        if y < H:
            spots.append((128 + y, CY + H + y))
        if y >= CY - H:
            spots.append((128 + y, y - (CY - H)))
        for re, s in spots:
            im = re + CY
            fwd[re, :WIN] = ya[:, s]
            fwd[im, :WIN] = yb[:, s]
            fwd[im, 128 : 128 + WIN] = ya[:, s]
            fwd[re, 128 : 128 + WIN] = -yb[:, s]
            inv[:WIN, re] = yc[s, :]
            inv[128 : 128 + WIN, re] = -yd[s, :]
            inv[128 : 128 + WIN, im] = yc[s, :]
            inv[:WIN, im] = yd[s, :]
    return fwd, inv


MIB = 1024 * 1024
ROWS = 40


def limit(mib):
    return pltpu.CompilerParams(vmem_limit_bytes=int(mib * MIB))


def lane_flags(mask_ref):
    even = mask_ref[pl.ds(0, 16, stride=2), :]
    odd = mask_ref[pl.ds(1, 16, stride=2), :]
    return jnp.concatenate([even, odd], axis=1).astype(F32)


def make_time_table(table_ref):
    f = FLO + lax.broadcasted_iota(jnp.int32, (NF, 128), 0)
    n = lax.broadcasted_iota(jnp.int32, (NF, 128), 1)
    fine = (f * n % NT).astype(F32) * (2.0 * np.pi / NT)
    coarse = (f * n % (NT // 128)).astype(F32) * (2.0 * np.pi * 128 / NT)
    cos_fine, sin_fine = jnp.cos(fine), jnp.sin(fine)
    cos_coarse, sin_coarse = jnp.cos(coarse), jnp.sin(coarse)
    for u in range(NT // 128):
        c, s = cos_coarse[:, u : u + 1], sin_coarse[:, u : u + 1]
        at = u * 128
        table_ref[:NF, at : at + 128] = (c * cos_fine - s * sin_fine).astype(BF16)
        table_ref[NF:, at : at + 128] = (-(s * cos_fine + c * sin_fine)).astype(BF16)


def spectra_kernel(record_ref, hold_ref, in_ref, table_ref, sems):
    chunk, ahead = 8, 4
    chunks = CX // chunk

    def copy(i):
        part = pl.ds(i * chunk, chunk)
        return pltpu.make_async_copy(record_ref.at[part], in_ref.at[part], sems.at[i])

    for i in range(ahead):
        copy(i).start()
    make_time_table(table_ref)

    def transform(i, carry):
        copy(i).wait()

        traces = in_ref[pl.ds(i * chunk, chunk)].reshape(-1, NT)
        res = lax.dot_general(
            table_ref[...], traces, (((1,), (1,)), ((), ())), preferred_element_type=F32
        )
        for b in range(chunk // 2):
            row = i * (chunk // 2) + b
            at = pl.ds(pl.multiple_of(row * PAD, 8), 2 * NF)
            hold_ref[at, :] = res[:, b * 128 : (b + 1) * 128]
        return carry

    lax.fori_loop(0, chunks, transform, 0)


def place_kernel(hold_ref, mask_ref, out_ref):
    flags = lane_flags(mask_ref)
    kept = flags > 0
    halves = [flags[c * 8 : (c + 1) * 8].astype(BF16) for c in range(2)]

    def place(group, carry):
        for k in range(16):
            f = group * 16 + k
            for p in range(2):
                part = hold_ref[pl.ds(p * NF + f, 16, stride=PAD), :]
                out_ref[f, p * 16 : (p + 1) * 16, :] = jnp.where(kept, part, 0.0).astype(BF16)
            out_ref[f, 32:40, :] = halves[k // 8]
        return carry

    lax.fori_loop(0, NF // 16, place, 0)


def spectra_of(record, sampled):
    hold = pl.pallas_call(
        spectra_kernel,
        in_specs=[pl.BlockSpec(memory_space=pltpu.HBM)],
        out_specs=VMEM,
        out_shape=jax.ShapeDtypeStruct((16 * PAD, 128), F32),
        scratch_shapes=[
            pltpu.VMEM((CX, CY, NT), BF16),
            pltpu.VMEM((2 * NF, NT), BF16),
            pltpu.SemaphoreType.DMA((CX // 8,)),
        ],
        compiler_params=limit(51),
        name="spectra",
    )(record)
    return pl.pallas_call(
        place_kernel,
        in_specs=[VMEM, VMEM],
        out_specs=VMEM,
        out_shape=jax.ShapeDtypeStruct((NF, ROWS, 128), BF16),
        compiler_params=limit(40),
        name="place",
    )(hold, sampled)


GROUP = 4


def early_lanes(rows):
    return lax.broadcasted_iota(jnp.int32, (rows, 128), 1) % CY < CY // 2


def low_lanes():
    return lax.broadcasted_iota(jnp.int32, (QUARTER, 128), 1) < CY


def side_by_side(blocks):
    return jnp.concatenate(blocks, axis=1)


def columns_of(in_ref, ry, p):
    return in_ref[:, ry, p * 16 : (p + 1) * 16, :].reshape(HALF, 128)


def forward_columns(parts, fx_ref, tw_ref, v_ref, start):
    low = low_lanes()
    for odd in range(2):
        upper, lower = [x[:QUARTER] for x in parts], [x[QUARTER:] for x in parts]
        data = jnp.concatenate([u - w if odd else u + w for u, w in zip(upper, lower)], axis=0)
        table = fx_ref[odd * HALF : (odd + 1) * HALF]
        res = jnp.dot(table, data, preferred_element_type=F32)
        rows = odd * QUARTER
        tr = tw_ref[rows : rows + QUARTER]
        ti = tw_ref[HALF + rows : HALF + rows + QUARTER]
        for k in range(GROUP):
            at = k * 128
            ar, ai = res[:QUARTER, at : at + 128], res[QUARTER:, at : at + 128]
            br = ar * tr - ai * ti
            bi = ar * ti + ai * tr
            first = jnp.where(low, br, pltpu.roll(bi, CY, 1))
            second = jnp.where(low, pltpu.roll(br, CY, 1), bi)
            v_ref[start + k, rows : rows + QUARTER] = (first + second).astype(BF16)
            v_ref[start + k, HALF + rows : HALF + rows + QUARTER] = (first - second).astype(BF16)


def forward_tiles(v_ref, wf_ref, c_ref):
    early = early_lanes(LX)
    best = jnp.zeros((8, 128), F32)
    for j in range(TILES):
        left, right = (j + TILES - 1) % TILES, (j + 1) % TILES
        near = jnp.where(early, v_ref[right], v_ref[left])
        c = jnp.dot(side_by_side([v_ref[j], near]), wf_ref[...], preferred_element_type=F32)
        c_ref[j] = c
        squares = c[:, :128] * c[:, :128] + c[:, 128:] * c[:, 128:]
        best = jnp.maximum(best, jnp.max(squares.reshape(-1, 8, 128), axis=0))
    return best


def put_largest(best, top_ref):
    top = jnp.sqrt(jnp.max(best, keepdims=True))
    top_ref[...] = jnp.broadcast_to(top, top_ref.shape)


def shrink_tiles(c_ref, tops_ref, level, wi_ref, o_ref):
    tau = level.astype(F32) * 0.001 * (
        jnp.max(tops_ref[...], axis=0, keepdims=True) + 1e-06
    )
    for j in range(TILES):
        real, imag = c_ref[j, :, :128], c_ref[j, :, 128:]
        g = jnp.maximum(1.0 - tau * lax.rsqrt(real * real + imag * imag), 0.0)
        e = side_by_side([real * g, imag * g]).astype(BF16)
        o_ref[j] = jnp.dot(e, wi_ref[...], preferred_element_type=F32)


def inverse_columns(o_ref, ix_ref, tw_ref, start):
    low, early = low_lanes(), early_lanes(QUARTER)
    made = []
    for odd in range(2):
        rows = odd * QUARTER
        tr = tw_ref[rows : rows + QUARTER]
        ti = tw_ref[HALF + rows : HALF + rows + QUARTER]
        reals, imags = [], []
        for j in range(start, start + GROUP):
            left, right = (j + TILES - 1) % TILES, (j + 1) % TILES
            halves = []
            for at in (rows, HALF + rows):
                part = pl.ds(at, QUARTER)
                near = jnp.where(early, o_ref[left, part, 128:], o_ref[right, part, 128:])
                halves.append(o_ref[j, part, :128] + near)
            total, apart = halves[0] + halves[1], halves[0] - halves[1]
            real = jnp.where(low, total, pltpu.roll(apart, CY, 1))
            imag = jnp.where(low, pltpu.roll(total, CY, 1), apart)
            reals.append((real * tr + imag * ti).astype(BF16))
            imags.append((imag * tr - real * ti).astype(BF16))
        g = jnp.concatenate([side_by_side(reals), side_by_side(imags)], axis=0)
        table = ix_ref[odd * HALF : (odd + 1) * HALF]
        made.append(jnp.dot(table, g, preferred_element_type=F32))
    even, odd = made
    return [
        jnp.concatenate([even[at : at + QUARTER] + odd[at : at + QUARTER],
                         even[at : at + QUARTER] - odd[at : at + QUARTER]], axis=0).astype(BF16)
        for at in (0, QUARTER)
    ]


def first_kernel(in_ref, fx_ref, tw_ref, wf_ref, c_ref, top_ref, v_ref):
    for start in range(0, TILES, GROUP):
        parts = [
            side_by_side([columns_of(in_ref, start + k, p) for k in range(GROUP)])
            for p in range(2)
        ]
        forward_columns(parts, fx_ref, tw_ref, v_ref, start)
    put_largest(forward_tiles(v_ref, wf_ref, c_ref), top_ref)


def middle_kernel(
    level_ref, core_ref, c_ref, tops_ref, in_ref, flag_ref, fx_ref, ix_ref, tw_ref, wf_ref, wi_ref,
    c2_ref, top_ref, o_ref, v_ref,
):
    shrink_tiles(c_ref, tops_ref, level_ref[0], wi_ref, o_ref)
    on_first = core_ref[0] == 0
    for start in range(0, TILES, GROUP):
        fresh = inverse_columns(o_ref, ix_ref, tw_ref, start)
        kept = []
        for k in range(GROUP):
            mine = in_ref[:, start + k, 32:40, :]
            other = flag_ref[:, start + k]
            upper, lower = jnp.where(on_first, mine, other), jnp.where(on_first, other, mine)
            kept.append(jnp.concatenate([upper, lower], axis=1).reshape(HALF, 128))
        kept = side_by_side(kept) > 0
        parts = []
        for p in range(2):
            sent = side_by_side([columns_of(in_ref, start + k, p) for k in range(GROUP)])
            parts.append(jnp.where(kept, sent, fresh[p]))
        forward_columns(parts, fx_ref, tw_ref, v_ref, start)
    put_largest(forward_tiles(v_ref, wf_ref, c2_ref), top_ref)


def last_kernel(level_ref, c_ref, tops_ref, ix_ref, tw_ref, wi_ref, out_ref, o_ref):
    shrink_tiles(c_ref, tops_ref, level_ref[1], wi_ref, o_ref)
    for start in range(0, TILES, GROUP):
        fresh = inverse_columns(o_ref, ix_ref, tw_ref, start)
        for k in range(GROUP):
            for p in range(2):
                part = fresh[p][:, k * 128 : (k + 1) * 128]
                out_ref[:, start + k, p * 16 : (p + 1) * 16, :] = part.reshape(NRX, 16, 128)


COEFFS = jax.ShapeDtypeStruct((TILES, LX, 256), F32)
TOPS = jax.ShapeDtypeStruct((NF, 128), F32)
V_SCRATCH = pltpu.VMEM((TILES, LX, 128), BF16)
O_SCRATCH = pltpu.VMEM((TILES, LX, 256), F32)


def first_half(arrived, fx, tw, wf):
    return pl.pallas_call(
        first_kernel,
        in_specs=[VMEM] * 4,
        out_specs=[VMEM] * 2,
        out_shape=[COEFFS, TOPS],
        scratch_shapes=[V_SCRATCH],
        compiler_params=limit(18),
        name="first",
    )(arrived, fx, tw, wf)


def middle(levels, core, c, tops, arrived, flags, fx, ix, tw, wf, wi):
    return pl.pallas_call(
        middle_kernel,
        in_specs=[SMEM] * 2 + [VMEM] * 9,
        out_specs=[VMEM] * 2,
        out_shape=[COEFFS, TOPS],
        scratch_shapes=[O_SCRATCH, V_SCRATCH],
        compiler_params=limit(26),
        name="middle",
    )(levels, core, c, tops, arrived, flags, fx, ix, tw, wf, wi)


def last_half(levels, c, tops, ix, tw, wi):
    return pl.pallas_call(
        last_kernel,
        in_specs=[SMEM] + [VMEM] * 5,
        out_specs=VMEM,
        out_shape=jax.ShapeDtypeStruct((NRX, TILES, 32, 128), BF16),
        scratch_shapes=[O_SCRATCH],
        compiler_params=limit(18),
        name="last",
    )(levels, c, tops, ix, tw, wi)


CHUNK = 4
CHUNKS = CX // CHUNK


def rebuild_kernel(in_ref, record_ref, mask_ref, table_ref, out_ref, made_ref, hold_ref, sems):
    def spread(group, carry):
        for k in range(8):
            f = group * 8 + k
            at = pl.ds(pl.multiple_of(f * PAD3, 8), 32)
            hold_ref[at, :] = in_ref[f].astype(F32) * (2.0 / NT)
        return carry

    lax.fori_loop(0, NF // 8, spread, 0, unroll=4)
    flags = lane_flags(mask_ref)

    def copy(i):
        part = pl.ds(i * CHUNK, CHUNK)
        return pltpu.make_async_copy(made_ref.at[part], out_ref.at[part], sems.at[i])

    for i in range(CHUNKS):
        first = i * CHUNK // 2
        rows = range(first, first + CHUNK // 2)
        spec = side_by_side(
            [
                jnp.concatenate(
                    [hold_ref[pl.ds(p * 16 + row, NF, stride=PAD3), :] for p in range(2)], axis=0
                )
                for row in rows
            ]
        ).astype(BF16)
        recon = lax.dot_general(
            spec, table_ref[...], (((0,), (0,)), ((), ())), preferred_element_type=F32
        )
        for k, row in enumerate(rows):
            kept = jnp.transpose(jnp.broadcast_to(flags[row : row + 1], (128, 128))) > 0
            for t in range(0, NT, 128):
                rec = record_ref[2 * row : 2 * row + 2, :, t : t + 128].reshape(128, 128)
                new = recon[k * 128 : (k + 1) * 128, t : t + 128].astype(BF16)
                mixed = jnp.where(kept, rec, new).reshape(2, CY, 128)
                made_ref[2 * row : 2 * row + 2, :, t : t + 128] = mixed
        copy(i).start()
    for i in range(CHUNKS):
        copy(i).wait()


def rebuild(returned, record, sampled, table):
    return pl.pallas_call(
        rebuild_kernel,
        in_specs=[VMEM] * 4,
        out_specs=pl.BlockSpec(memory_space=pltpu.HBM),
        out_shape=jax.ShapeDtypeStruct((CX, CY, NT), BF16),
        scratch_shapes=[
            pltpu.VMEM((CX, CY, NT), BF16),
            pltpu.VMEM((NF * PAD3, 128), F32),
            pltpu.SemaphoreType.DMA((CHUNKS,)),
        ],
        compiler_params=limit(26),
        name="rebuild",
    )(returned, record, sampled, table)


def exchange(array):
    return lax.all_to_all(array, ALL, split_axis=0, concat_axis=0, tiled=True)


def all_tops(top):
    return exchange(top.reshape(NF, 1, 128)).reshape(NF, 128)


def tables():
    fx, ix = plane_tables()
    wf, wi = window_tables()
    narrow = [np.asarray(t, jnp.bfloat16) for t in (time_table(), fx, ix, wf, wi)]
    return (*narrow, np.asarray(twiddle_table(), np.float32))


def body(record, sampled, levels):
    time, fx, ix, wf, wi, tw = tables()
    sent = spectra_of(record, sampled)
    arrived = exchange(sent).reshape(NRX, TILES, ROWS, 128)
    flags = lax.ppermute(arrived[:, :, 32:40, :], ALL[2], [(0, 1), (1, 0)])
    c, top = first_half(arrived, fx, tw, wf)
    core = lax.axis_index(ALL[2]).reshape(1)
    top, flags, core = lax.optimization_barrier((top, flags, core))
    c, top = middle(levels, core, c, all_tops(top), arrived, flags, fx, ix, tw, wf, wi)
    back = last_half(levels, c, all_tops(top), ix, tw, wi)
    returned = exchange(back.reshape(NF, 32, 128))
    return rebuild(returned, record, sampled, time)


def solution(mesh):
    finer = Mesh(mesh.devices.reshape(2, 4, 2, 2, 4), ALL)
    rx, ry = ALL[:3], ALL[3:]
    return jax.shard_map(
        body,
        mesh=finer,
        in_specs=(P(rx, ry, None), P(rx, ry), P()),
        out_specs=P(rx, ry, None),
        check_vma=False,
    )
```
